64 devices in a mesh: dp: 8 (over x, y, core), tp: 8 (over z).
Axes of the slice: x: 2, y: 2, z: 8, core: 2. Of those that a mesh axis runs over, the one named last changes fastest.
The devices are a block of a 4x4x8 slice.
Arguments:
- x: bfloat16 [16384, 2560], P('dp'), parts along dimension 0
- dy: bfloat16 [16384, 2560], P('dp'), parts along dimension 0
- gate: bfloat16 [16384, 10240], P('dp', 'tp'), parts along dimension 0
- up: bfloat16 [16384, 10240], P('dp', 'tp'), parts along dimension 0
- w_gate: bfloat16 [2560, 10240], P(None, 'tp')
- w_up: bfloat16 [2560, 10240], P(None, 'tp')
- w_down: bfloat16 [10240, 2560], P('tp')
Outputs:
- output 1: bfloat16 [16384, 2560], P('dp'), parts along dimension 0
- output 2: bfloat16 [20480, 10240], P('dp', 'tp'), parts along dimension 0
- output 3: bfloat16 [20480, 10240], P('dp', 'tp'), parts along dimension 0
- output 4: bfloat16 [81920, 2560], P(('dp', 'tp')), parts along dimension 0
There are 8 independent parts. The reference program is written for one: setup_inputs(seed, part) draws one part's arguments, and reference() takes and returns one part's arrays. A program takes and returns all parts, laid end to end along the dimension named above; an argument that names none is the same for every part.
All inputs are finite; a program needn't handle non-finite values.
Results may differ from the reference program's by a relative error of at most 0.012.
Values are sent between devices in bfloat16 or wider.
A program may use at most 768 MiB of HBM per device.

```python
import jax
import jax.numpy as jnp

ROWS = 2048
D = 2560
FF = 10240


def act(gate, up):
    return jax.nn.gelu(gate) * up


def setup_inputs(seed: int = 0, part: int = 0) -> dict:
    kx, ky, ka, kb, kg, ku, kd = jax.random.split(jax.random.key(seed), 7)
    kx, ky, ka, kb = (jax.random.fold_in(k, part) for k in (kx, ky, ka, kb))
    drawn = {
        "x": jax.random.normal(kx, (ROWS, D), jnp.float32),
        "dy": jax.random.normal(ky, (ROWS, D), jnp.float32),
        "gate": jax.random.normal(ka, (ROWS, FF), jnp.float32),
        "up": jax.random.normal(kb, (ROWS, FF), jnp.float32),
        "w_gate": jax.random.normal(kg, (D, FF), jnp.float32) * D**-0.5,
        "w_up": jax.random.normal(ku, (D, FF), jnp.float32) * D**-0.5,
        "w_down": jax.random.normal(kd, (FF, D), jnp.float32) * FF**-0.5,
    }
    return {k: v.astype(jnp.bfloat16) for k, v in drawn.items()}


def reference(x, dy, gate, up, w_gate, w_up, w_down):
    hidden, back = jax.vjp(act, gate.astype(jnp.float32), up.astype(jnp.float32))
    d_hidden = jnp.dot(dy, w_down.T, preferred_element_type=jnp.float32)
    d_gate, d_up = (g.astype(jnp.bfloat16) for g in back(d_hidden))
    dx = jnp.dot(d_gate, w_gate.T, preferred_element_type=jnp.float32) + jnp.dot(d_up, w_up.T, preferred_element_type=jnp.float32)
    dw_gate = jnp.dot(x.T, d_gate, preferred_element_type=jnp.float32)
    dw_up = jnp.dot(x.T, d_up, preferred_element_type=jnp.float32)
    dw_down = jnp.dot(hidden.astype(jnp.bfloat16).T, dy, preferred_element_type=jnp.float32)
    return tuple(g.astype(jnp.bfloat16) for g in (dx, dw_gate, dw_up, dw_down))
```

```python
import functools

import jax
import jax.numpy as jnp
from jax import lax
from jax.experimental import pallas as pl
from jax.experimental.pallas import tpu as pltpu
from jax.sharding import PartitionSpec as P

BF = jnp.bfloat16
F32 = jnp.float32
W = 256
MESH = pl.DeviceIdType.MESH
ROOT = 0.7978845608028654
CUBE = 0.044715


def nt(a, b):
    return lax.dot_general(a, b, (((1,), (1,)), ((), ())), preferred_element_type=F32)


def tn(a, b):
    return lax.dot_general(a, b, (((0,), (0,)), ((), ())), preferred_element_type=F32)


def kernel(n, x, dy, gate, up, wg, wu, wd, dx, dwg, dwu, dwd,
           dy_v, dgu, hid, wd_v, wgu, buf, xt, ost,
           rs_send, rs_recv, ag_send, ag_recv, in_sem, wd_sem, w_sem, own_sem, x_sem, o_sem):
    T, D = x.shape
    F = gate.shape[1]
    R = T // n
    H = D // 2
    C = H // W
    FT = F // W
    me = lax.axis_index("tp")
    right, left = lax.rem(me + 1, n), lax.rem(me + n - 1, n)
    to = (right, left)

    def mod(b):
        return lax.rem(b + 2 * n, n)

    def ds(i, size):
        return pl.ds(pl.multiple_of(i * size, size), size)

    def load_block(b):
        rows = ds(b, R)
        return (pltpu.make_async_copy(dy.at[rows, :], dy_v.at[rows, :], in_sem.at[0, b]),
                pltpu.make_async_copy(gate.at[rows, :], dgu.at[0, rows, :], in_sem.at[1, b]),
                pltpu.make_async_copy(up.at[rows, :], dgu.at[1, rows, :], in_sem.at[2, b]))

    def load_wd(j):
        return pltpu.make_async_copy(wd.at[ds(j, W), :], wd_v.at[ds(j, W), :], wd_sem.at[j])

    def load_w(t):
        return (pltpu.make_async_copy(wg.at[ds(t, W), :], wgu.at[0, ds(t, W), :], w_sem.at[0, t]),
                pltpu.make_async_copy(wu.at[ds(t, W), :], wgu.at[1, ds(t, W), :], w_sem.at[1, t]))

    def load_x(i, k):
        return pltpu.make_async_copy(x.at[:, ds(i, W)], xt.at[k], x_sem.at[k])

    def rs(d, s, j):
        return pltpu.make_async_remote_copy(
            src_ref=buf.at[d, s, j], dst_ref=buf.at[d, s + 1, j],
            send_sem=rs_send.at[d, s, j], recv_sem=rs_recv.at[d, s, j],
            device_id={"tp": to[d]}, device_id_type=MESH)

    def rs_block(d, s):
        return mod(me - 1 - s) if d == 0 else mod(me - 1 + s)

    def piece(d, b, j):
        return dx.at[ds(b, R), ds(d * C + j, W)]

    def ag_first(d, j):
        b = rs_block(d, n - 1)
        return pltpu.make_async_remote_copy(
            src_ref=buf.at[d, n - 1, j], dst_ref=piece(d, b, j),
            send_sem=ag_send.at[d, 0, j], recv_sem=ag_recv.at[d, 0, j],
            device_id={"tp": to[d]}, device_id_type=MESH)

    def ag_own(d, j):
        return pltpu.make_async_copy(buf.at[d, n - 1, j], piece(d, rs_block(d, n - 1), j), own_sem.at[d, j])

    def ag(d, a, j, b):
        return pltpu.make_async_remote_copy(
            src_ref=piece(d, b, j), dst_ref=piece(d, b, j),
            send_sem=ag_send.at[d, a, j], recv_sem=ag_recv.at[d, a, j],
            device_id={"tp": to[d]}, device_id_type=MESH)

    def ag_in(d, a):
        return mod(me - 1 - a) if d == 0 else mod(me - 1 + a)

    def wait_block(b):
        for c in load_block(b):
            c.wait()

    def dh(b, j):
        rows, cols = ds(b, R), ds(j, W)
        d = nt(dy_v[rows, :], wd_v[cols, :])
        g = dgu[0, rows, cols].astype(F32)
        u = dgu[1, rows, cols].astype(F32)
        g2 = g * g
        t = jnp.tanh(ROOT * (g + CUBE * (g2 * g)))
        cdf = 0.5 * (1.0 + t)
        act = g * cdf
        slope = cdf + g * (0.5 * (1.0 - t * t)) * (ROOT * (1.0 + (3.0 * CUBE) * g2))
        hid[rows, cols] = (act * u).astype(BF)
        dgu[0, rows, cols] = (d * u * slope).astype(BF)
        dgu[1, rows, cols] = (d * act).astype(BF)

    def term(d, s, j):
        rows, tile = ds(rs_block(d, s), R), ds(d * C + j, W)
        return nt(dgu[0, rows, :], wgu[0, tile, :]) + nt(dgu[1, rows, :], wgu[1, tile, :])

    def rs_slot(s, j, first=False, last=False, blocks=()):
        if first:
            for d in (0, 1):
                for c in load_w(d * C + j):
                    c.wait()
        else:
            for d in (0, 1):
                rs(d, s - 1, j).wait_recv()
        if blocks:
            @pl.when(j == 0)
            def _():
                for b in blocks:
                    wait_block(b)
        sums = [term(d, s, j) for d in (0, 1)]
        if not first:
            sums = [buf[d, s, j].astype(F32) + sums[d] for d in (0, 1)]
        for d in (0, 1):
            buf[d, s, j] = sums[d].astype(BF)
        for d in (0, 1):
            if last:
                ag_first(d, j).start()
                ag_own(d, j).start()
            else:
                rs(d, s, j).start()
        for b in blocks:
            dh(b, j)

    order = [mod(me - 1), mod(me - 2), me, mod(me - 3), mod(me + 1), mod(me - 4), mod(me + 2), mod(me + 3)]
    for c in load_block(order[0]):
        c.start()
    for j in range(FT):
        load_wd(j).start()
    for j in range(C):
        for d in (0, 1):
            for c in load_w(d * C + j):
                c.start()
    for b in order[1:]:
        for c in load_block(b):
            c.start()
    for k in (0, 1):
        load_x(k, k).start()

    barrier = pltpu.get_barrier_semaphore()
    for p in (left, right):
        pl.semaphore_signal(barrier, inc=1, device_id={"tp": p}, device_id_type=MESH)
    pl.semaphore_wait(barrier, 2)

    wait_block(order[0])

    @pl.loop(0, FT)
    def _(j):
        load_wd(j).wait()
        dh(order[0], j)

    @pl.loop(0, C)
    def _(j):
        rs_slot(0, j, first=True, blocks=(mod(me - 2), me))

    @pl.loop(0, 2 * C)
    def _(q):
        s, j = q // C + 1, lax.rem(q, C)
        rs_slot(s, j, blocks=(mod(me - 2 - s), mod(me + s)))

    @pl.loop(0, C)
    def _(j):
        rs_slot(3, j, blocks=(mod(me + 3),))

    @pl.loop(0, (n - 5) * C)
    def _(q):
        rs_slot(q // C + 4, lax.rem(q, C))

    @pl.loop(0, C)
    def _(j):
        rs_slot(n - 1, j, last=True)

    @pl.loop(0, (n - 1) * C)
    def _(q):
        for d in (0, 1):
            rs(d, q // C, lax.rem(q, C)).wait_send()

    def forward(q):
        a, j = q // C, lax.rem(q, C)
        for d in (0, 1):
            b = ag_in(d, a)
            ag(d, a, j, b).wait_recv()

            @pl.when(a < n - 2)
            def _():
                ag(d, a + 1, j, b).start()

    def put(k, dst):
        return pltpu.make_async_copy(ost.at[k], dst, o_sem.at[k])

    @pl.loop(0, D // W)
    def _(i):
        k = lax.rem(i, 2)
        load_x(i, k).wait()
        for h, out in ((0, dwg), (1, dwu)):
            @pl.when(i > 0)
            def _():
                put(h, out.at[ds(i - 1, W), :]).wait()
            ost[h] = tn(xt[k], dgu[h]).astype(BF)
            put(h, out.at[ds(i, W), :]).start()
            forward(2 * i + h)

        @pl.when(i + 2 < D // W)
        def _():
            load_x(i + 2, k).start()

    @pl.loop(0, FT)
    def _(i):
        for h in (0, 1):
            put(h, dwd.at[ds(0, W), ds(h, H)]).wait()
            ost[h] = tn(hid[:, ds(i, W)], dy_v[:, h * H:(h + 1) * H]).astype(BF)
            put(h, dwd.at[ds(i, W), ds(h, H)]).start()
            forward(2 * (D // W) + 2 * i + h)

    @pl.loop(2 * (D // W) + 2 * FT, (n - 1) * C)
    def _(q):
        forward(q)

    for h in (0, 1):
        put(h, dwd.at[ds(0, W), ds(h, H)]).wait()

    @pl.loop(0, C)
    def _(j):
        for d in (0, 1):
            ag_own(d, j).wait()
            ag_first(d, j).wait_send()

    @pl.loop(C, (n - 1) * C)
    def _(q):
        for d in (0, 1):
            ag(d, q // C, lax.rem(q, C), me).wait_send()


def solution(mesh):
    n = mesh.shape["tp"]

    def step(x, dy, gate, up, w_gate, w_up, w_down):
        T, D = x.shape
        F = gate.shape[1]
        R, C, FT = T // n, D // 2 // W, F // W
        assert C == FT and n == 8
        dma = pltpu.SemaphoreType.DMA
        any_ = pl.BlockSpec(memory_space=pl.ANY)
        return pl.pallas_call(
            functools.partial(kernel, n),
            out_shape=[jax.ShapeDtypeStruct(s, BF) for s in ((T, D), (D, F), (D, F), (F, D))],
            in_specs=[any_] * 7,
            out_specs=[any_] * 4,
            scratch_shapes=[
                pltpu.VMEM((T, D), BF),
                pltpu.VMEM((2, T, F), BF),
                pltpu.VMEM((T, F), BF),
                pltpu.VMEM((F, D), BF),
                pltpu.VMEM((2, D, F), BF),
                pltpu.VMEM((2, n, C, R, W), BF),
                pltpu.VMEM((2, T, W), BF),
                pltpu.VMEM((2, W, F), BF),
                dma((2, n - 1, C)), dma((2, n - 1, C)), dma((2, n - 1, C)), dma((2, n - 1, C)),
                dma((3, n)), dma((FT,)), dma((2, 2 * C)), dma((2, C)), dma((2,)), dma((2,)),
            ],
            compiler_params=pltpu.CompilerParams(
                collective_id=0, has_side_effects=True, vmem_limit_bytes=67043328),
            name="mlp_bwd",
        )(x, dy, gate, up, w_gate, w_up, w_down)

    tokens, columns, rows = P("dp", None), P(None, "tp"), P("tp", None)
    return jax.shard_map(
        step,
        mesh=mesh,
        in_specs=(tokens, tokens, P("dp", "tp"), P("dp", "tp"), columns, columns, rows),
        out_specs=(tokens, P("dp", "tp"), P("dp", "tp"), P(("dp", "tp"), None)),
        check_vma=False,
    )
```

```python
import functools

import jax
import jax.numpy as jnp
from jax import lax
from jax.experimental import pallas as pl
from jax.experimental.pallas import tpu as pltpu
from jax.sharding import PartitionSpec as P

BF = jnp.bfloat16
F32 = jnp.float32
W = 256
MESH = pl.DeviceIdType.MESH
ROOT = 0.7978845608028654
CUBE = 0.044715


def nt(a, b):
    return lax.dot_general(a, b, (((1,), (1,)), ((), ())), preferred_element_type=F32)


def tn(a, b):
    return lax.dot_general(a, b, (((0,), (0,)), ((), ())), preferred_element_type=F32)


def kernel(n, x, dy, gate, up, wg, wu, wd, dx, end_r, end_l, dwg, dwu, dwd,
           dy_v, dgu, hid, buf, xt,
           rs_send, rs_recv, ag_send, ag_recv, in_sem, wd_sem, w_sem, own_sem, x_sem):
    T, D = x.shape
    F = gate.shape[1]
    R = T // n
    H = D // 2
    C = H // W
    FT = F // W
    me = lax.axis_index("tp")
    right, left = lax.rem(me + 1, n), lax.rem(me + n - 1, n)
    to = (right, left)

    def mod(b):
        return lax.rem(b + 2 * n, n)

    def ds(i, size):
        return pl.ds(pl.multiple_of(i * size, size), size)

    def load_block(b):
        rows = ds(b, R)
        return (pltpu.make_async_copy(dy.at[rows, :], dy_v.at[rows, :], in_sem.at[0, b]),
                pltpu.make_async_copy(gate.at[rows, :], dgu.at[0, rows, :], in_sem.at[1, b]),
                pltpu.make_async_copy(up.at[rows, :], dgu.at[1, rows, :], in_sem.at[2, b]))

    def load_wd(j):
        return pltpu.make_async_copy(wd.at[ds(j, W), :], dwd.at[ds(j, W), :], wd_sem.at[j])

    def load_w(t):
        return (pltpu.make_async_copy(wg.at[ds(t, W), :], dwg.at[ds(t, W), :], w_sem.at[0, t]),
                pltpu.make_async_copy(wu.at[ds(t, W), :], dwu.at[ds(t, W), :], w_sem.at[1, t]))

    def load_x(i, k):
        return pltpu.make_async_copy(x.at[:, ds(i, W)], xt.at[k], x_sem.at[k])

    def rs(d, s, j):
        return pltpu.make_async_remote_copy(
            src_ref=buf.at[d, s, j], dst_ref=buf.at[d, s + 1, j],
            send_sem=rs_send.at[d, s, j], recv_sem=rs_recv.at[d, s, j],
            device_id={"tp": to[d]}, device_id_type=MESH)

    def rs_block(d, s):
        return mod(me - 1 - s) if d == 0 else mod(me - 1 + s)

    def piece(d, b, j):
        return dx.at[ds(b, R), ds(d * C + j, W)]

    def ag_first(d, j):
        b = rs_block(d, n - 1)
        return pltpu.make_async_remote_copy(
            src_ref=buf.at[d, n - 1, j], dst_ref=piece(d, b, j),
            send_sem=ag_send.at[d, 0, j], recv_sem=ag_recv.at[d, 0, j],
            device_id={"tp": to[d]}, device_id_type=MESH)

    def ag_own(d, j):
        return pltpu.make_async_copy(buf.at[d, n - 1, j], piece(d, rs_block(d, n - 1), j), own_sem.at[d, j])

    def ag(d, a, j, b):
        return pltpu.make_async_remote_copy(
            src_ref=piece(d, b, j), dst_ref=piece(d, b, j),
            send_sem=ag_send.at[d, a, j], recv_sem=ag_recv.at[d, a, j],
            device_id={"tp": to[d]}, device_id_type=MESH)

    def ag_end(d, j, b):
        return pltpu.make_async_remote_copy(
            src_ref=piece(d, b, j), dst_ref=(end_r, end_l)[d].at[:, ds(j, W)],
            send_sem=ag_send.at[d, n - 3, j], recv_sem=ag_recv.at[d, n - 3, j],
            device_id={"tp": to[d]}, device_id_type=MESH)

    def ag_in(d, a):
        return mod(me - 1 - a) if d == 0 else mod(me - 1 + a)

    def wait_block(b):
        for c in load_block(b):
            c.wait()

    def dh(b, j):
        rows, cols = ds(b, R), ds(j, W)
        d = nt(dy_v[rows, :], dwd[cols, :])
        g = dgu[0, rows, cols].astype(F32)
        u = dgu[1, rows, cols].astype(F32)
        g2 = g * g
        t = jnp.tanh(ROOT * (g + CUBE * (g2 * g)))
        cdf = 0.5 * (1.0 + t)
        act = g * cdf
        slope = cdf + g * (0.5 * (1.0 - t * t)) * (ROOT * (1.0 + (3.0 * CUBE) * g2))
        hid[rows, cols] = (act * u).astype(BF)
        dgu[0, rows, cols] = (d * u * slope).astype(BF)
        dgu[1, rows, cols] = (d * act).astype(BF)

    def term(d, s, j):
        rows, tile = ds(rs_block(d, s), R), ds(d * C + j, W)
        return nt(dgu[0, rows, :], dwg[tile, :]) + nt(dgu[1, rows, :], dwu[tile, :])

    def rs_slot(s, j, first=False, last=False, blocks=()):
        if first:
            for d in (0, 1):
                for c in load_w(d * C + j):
                    c.wait()
        else:
            for d in (0, 1):
                rs(d, s - 1, j).wait_recv()
        if blocks:
            @pl.when(j == 0)
            def _():
                for b in blocks:
                    wait_block(b)
        sums = [term(d, s, j) for d in (0, 1)]
        if not first:
            sums = [buf[d, s, j].astype(F32) + sums[d] for d in (0, 1)]
        for d in (0, 1):
            buf[d, s, j] = sums[d].astype(BF)
        for d in (0, 1):
            if last:
                ag_first(d, j).start()
                ag_own(d, j).start()
            else:
                rs(d, s, j).start()
        for b in blocks:
            dh(b, j)

    order = [mod(me - 1), mod(me - 2), me, mod(me - 3), mod(me + 1), mod(me - 4), mod(me + 2), mod(me + 3)]

    def start(copies):
        for c in copies:
            c.start()

    def start_w(j):
        for d in (0, 1):
            start(load_w(d * C + j))

    start(load_block(order[0]))
    start([load_wd(j) for j in range(FT)])
    start_w(0)

    barrier = pltpu.get_barrier_semaphore()
    for p in (left, right):
        pl.semaphore_signal(barrier, inc=1, device_id={"tp": p}, device_id_type=MESH)
    pl.semaphore_wait(barrier, 2)

    wait_block(order[0])

    @pl.loop(0, FT)
    def _(j):
        load_wd(j).wait()

        @pl.when(j + 1 < C)
        def _():
            start_w(j + 1)
        for k in (0, 1):
            @pl.when(j == k)
            def _():
                start(load_block(order[k + 1]))
        dh(order[0], j)

    @pl.loop(0, C)
    def _(j):
        for k in range(5):
            @pl.when(j == k)
            def _():
                start(load_block(order[k + 3]))
        rs_slot(0, j, first=True, blocks=(mod(me - 2), me))

    @pl.loop(0, 2 * C)
    def _(q):
        s, j = q // C + 1, lax.rem(q, C)
        rs_slot(s, j, blocks=(mod(me - 2 - s), mod(me + s)))

    @pl.loop(0, C)
    def _(j):
        rs_slot(3, j, blocks=(mod(me + 3),))

    @pl.loop(0, (n - 5) * C)
    def _(q):
        rs_slot(q // C + 4, lax.rem(q, C))

    for k in (0, 1):
        load_x(k, k).start()

    @pl.loop(0, C)
    def _(j):
        rs_slot(n - 1, j, last=True)

    @pl.loop(0, (n - 1) * C)
    def _(q):
        for d in (0, 1):
            rs(d, q // C, lax.rem(q, C)).wait_send()

    def forward(q):
        a, j = q // C, lax.rem(q, C)
        for d in (0, 1):
            b = ag_in(d, a)

            @pl.when(a < n - 3)
            def _():
                ag(d, a, j, b).wait_recv()

            @pl.when(a < n - 4)
            def _():
                ag(d, a + 1, j, b).start()

            @pl.when(a == n - 4)
            def _():
                ag_end(d, j, b).start()

            @pl.when(a == n - 3)
            def _():
                ag_end(d, j, b).wait_recv()

    @pl.loop(0, D // W)
    def _(i):
        k = lax.rem(i, 2)
        load_x(i, k).wait()
        for h, out in ((0, dwg), (1, dwu)):
            out[ds(i, W), :] = tn(xt[k], dgu[h]).astype(BF)
            forward(2 * i + h)

        @pl.when(i + 2 < D // W)
        def _():
            load_x(i + 2, k).start()

    @pl.loop(0, FT)
    def _(i):
        for h in (0, 1):
            dwd[ds(i, W), h * H:(h + 1) * H] = tn(hid[:, ds(i, W)], dy_v[:, h * H:(h + 1) * H]).astype(BF)
            forward(2 * (D // W) + 2 * i + h)

    @pl.loop(0, C)
    def _(j):
        for d in (0, 1):
            ag_own(d, j).wait()
            ag_first(d, j).wait_send()
            ag_end(d, j, me).wait_send()

    @pl.loop(C, (n - 3) * C)
    def _(q):
        for d in (0, 1):
            ag(d, q // C, lax.rem(q, C), me).wait_send()


def half(ref, b, R, d):
    H = ref.shape[1] // 2
    return ref.at[pl.ds(pl.multiple_of(b * R, R), R), d * H:(d + 1) * H]


def copy_kernel(n, dx, end_r, end_l, dwg, dwu, dwd, dx_o, dwg_o, dwu_o, dwd_o, stage, in_sem, out_sem, w_sem):
    R = dx.shape[0] // n
    me = lax.axis_index("tp")
    parts = []
    for d, end in ((0, end_r), (1, end_l)):
        for a in range(-1, n - 2):
            b = lax.rem((me - 1 - a if d == 0 else me - 1 + a) + 2 * n, n)
            if d == 1 and a == -1:
                b = lax.rem(me - 2 + n, n)
            src = end if a == n - 3 else half(dx, b, R, d)
            i = len(parts)
            parts.append((pltpu.make_async_copy(src, stage.at[i], in_sem.at[i]),
                          pltpu.make_async_copy(stage.at[i], half(dx_o, b, R, d), out_sem.at[i])))
    whole = [pltpu.make_async_copy(v, o, w_sem.at[i])
             for i, (v, o) in enumerate(((dwg, dwg_o), (dwu, dwu_o), (dwd, dwd_o)))]
    for load, _ in parts:
        load.start()
    for c in whole:
        c.start()
    for load, store in parts:
        load.wait()
        store.start()
    for c in whole:
        c.wait()
    for _, store in parts:
        store.wait()


def end_kernel(n, dx, got_r, got_l, dx_o, sem):
    R = dx.shape[0] // n
    me = lax.axis_index("tp")
    copies = [pltpu.make_async_copy(got_r, half(dx_o, lax.rem(me + 1, n), R, 0), sem.at[0]),
              pltpu.make_async_copy(got_l, half(dx_o, lax.rem(me + n - 3, n), R, 1), sem.at[1])]
    for c in copies:
        c.start()
    for c in copies:
        c.wait()


def solution(mesh):
    n = mesh.shape["tp"]

    def step(x, dy, gate, up, w_gate, w_up, w_down):
        T, D = x.shape
        F = gate.shape[1]
        R, C, FT = T // n, D // 2 // W, F // W
        assert C == FT and n == 8
        dma = pltpu.SemaphoreType.DMA
        any_ = pl.BlockSpec(memory_space=pl.ANY)
        vmem = pl.BlockSpec(memory_space=pltpu.VMEM)
        hbm = pl.BlockSpec(memory_space=pltpu.HBM)
        shape = lambda *s: jax.ShapeDtypeStruct(s, BF)
        dws = [shape(D, F), shape(D, F), shape(F, D)]
        dx, end_r, end_l, *dw = pl.pallas_call(
            functools.partial(kernel, n),
            out_shape=[shape(T, D), shape(R, D // 2), shape(R, D // 2)] + [pltpu.VMEM(w.shape, BF) for w in dws],
            in_specs=[any_] * 7,
            out_specs=[any_] * 3 + [vmem] * 3,
            scratch_shapes=[
                pltpu.VMEM((T, D), BF),
                pltpu.VMEM((2, T, F), BF),
                pltpu.VMEM((T, F), BF),
                pltpu.VMEM((2, n, C, R, W), BF),
                pltpu.VMEM((2, T, W), BF),
                dma((2, n - 1, C)), dma((2, n - 1, C)), dma((2, n - 2, C)), dma((2, n - 2, C)),
                dma((3, n)), dma((FT,)), dma((2, 2 * C)), dma((2, C)), dma((2,)),
            ],
            compiler_params=pltpu.CompilerParams(
                collective_id=0, has_side_effects=True, vmem_limit_bytes=44 << 20),
            name="mlp_bwd",
        )(x, dy, gate, up, w_gate, w_up, w_down)
        ahead = [(i, (i + 1) % n) for i in range(n)]
        back = [(i, (i - 1) % n) for i in range(n)]
        got_r = lax.ppermute(end_r, "tp", ahead)
        got_l = lax.ppermute(end_l, "tp", back)
        m = 2 * (n - 1)
        dx, *dw = pl.pallas_call(
            functools.partial(copy_kernel, n),
            out_shape=[shape(T, D)] + dws,
            in_specs=[hbm] * 3 + [vmem] * 3,
            out_specs=[hbm] * 4,
            scratch_shapes=[pltpu.VMEM((m, R, D // 2), BF), dma((m,)), dma((m,)), dma((3,))],
            compiler_params=pltpu.CompilerParams(vmem_limit_bytes=10 << 20),
            cost_estimate=pl.CostEstimate(flops=13_000_000_000, bytes_accessed=41_000_000, transcendentals=0),
            name="place",
        )(*(pltpu.with_memory_space_constraint(v, pltpu.HBM) for v in (dx, end_r, end_l)), *dw)
        dx = pl.pallas_call(
            functools.partial(end_kernel, n),
            out_shape=shape(T, D),
            in_specs=[any_, vmem, vmem],
            out_specs=any_,
            scratch_shapes=[dma((2,))],
            input_output_aliases={0: 0},
            compiler_params=pltpu.CompilerParams(vmem_limit_bytes=1 << 20),
            name="place_end",
        )(dx, got_r, got_l)
        return dx, *dw

    tokens, columns, rows = P("dp", None), P(None, "tp"), P("tp", None)
    return jax.shard_map(
        step,
        mesh=mesh,
        in_specs=(tokens, tokens, P("dp", "tp"), P("dp", "tp"), columns, columns, rows),
        out_specs=(tokens, P("dp", "tp"), P("dp", "tp"), P(("dp", "tp"), None)),
        check_vma=False,
    )
```

```python
import functools

import jax
import jax.numpy as jnp
from jax import lax
from jax.experimental import pallas as pl
from jax.experimental.pallas import tpu as pltpu
from jax.sharding import PartitionSpec as P

BF = jnp.bfloat16
F32 = jnp.float32
W = 256
MESH = pl.DeviceIdType.MESH
ROOT = 0.7978845608028654
CUBE = 0.044715


def nt(a, b):
    return lax.dot_general(a, b, (((1,), (1,)), ((), ())), preferred_element_type=F32)


def tn(a, b):
    return lax.dot_general(a, b, (((0,), (0,)), ((), ())), preferred_element_type=F32)


def kernel(n, x, dy, gate, up, wg, wu, wd, dx, end_r, end_l, dwg, dwu, dwd,
           dy_v, dgu, hid, buf, xt,
           send_sem, recv_sem, credit, in_sem, wd_sem, w_sem, own_sem, x_sem):
    T, D = x.shape
    F = gate.shape[1]
    R = T // n
    H = D // 2
    C = H // W
    FT = F // W
    me = lax.axis_index("tp")
    right, left = lax.rem(me + 1, n), lax.rem(me + n - 1, n)
    to = (right, left)

    def mod(b):
        return lax.rem(b + 2 * n, n)

    def ds(i, size):
        return pl.ds(pl.multiple_of(i * size, size), size)

    def load_block(b):
        rows = ds(b, R)
        return (pltpu.make_async_copy(dy.at[rows, :], dy_v.at[rows, :], in_sem.at[0, b]),
                pltpu.make_async_copy(gate.at[rows, :], dgu.at[0, rows, :], in_sem.at[1, b]),
                pltpu.make_async_copy(up.at[rows, :], dgu.at[1, rows, :], in_sem.at[2, b]))

    def load_wd(j):
        return pltpu.make_async_copy(wd.at[ds(j, W), :], dwd.at[ds(j, W), :], wd_sem.at[j])

    def load_w(t):
        return (pltpu.make_async_copy(wg.at[ds(t, W), :], dwg.at[ds(t, W), :], w_sem.at[0, t]),
                pltpu.make_async_copy(wu.at[ds(t, W), :], dwu.at[ds(t, W), :], w_sem.at[1, t]))

    def load_x(i, k):
        return pltpu.make_async_copy(x.at[:, ds(i, W)], xt.at[k], x_sem.at[k])

    def hop(d, g, j, src, dst):
        k = lax.rem(g, 2)
        return pltpu.make_async_remote_copy(
            src_ref=src, dst_ref=dst, send_sem=send_sem.at[d, k, j], recv_sem=recv_sem.at[d, k, j],
            device_id={"tp": to[d]}, device_id_type=MESH)

    def rs(d, s, j):
        return hop(d, s, j, buf.at[d, s, j], buf.at[d, s + 1, j])

    def send(d, g, j, copy):
        def ready():
            hop(d, g, j, buf.at[d, 0, j], buf.at[d, 0, j]).wait_send()
            pl.semaphore_wait(credit.at[d], 1)

        if isinstance(g, int):
            if g >= 2:
                ready()
        else:
            pl.when(g >= 2)(ready)
        copy.start()

    def taken(d):
        pl.semaphore_signal(credit.at[d], inc=1, device_id={"tp": to[1 - d]}, device_id_type=MESH)

    def rs_block(d, s):
        return mod(me - 1 - s) if d == 0 else mod(me - 1 + s)

    def piece(d, b, j):
        return dx.at[ds(b, R), ds(d * C + j, W)]

    def ag_first(d, j):
        return hop(d, n - 1, j, buf.at[d, n - 1, j], piece(d, rs_block(d, n - 1), j))

    def ag_own(d, j):
        return pltpu.make_async_copy(buf.at[d, n - 1, j], piece(d, rs_block(d, n - 1), j), own_sem.at[d])

    def ag(d, a, j, b):
        return hop(d, a + n - 1, j, piece(d, b, j), piece(d, b, j))

    def ag_end(d, j, b):
        return hop(d, 2 * n - 4, j, piece(d, b, j), (end_r, end_l)[d].at[:, ds(j, W)])

    def ag_in(d, a):
        return mod(me - 1 - a) if d == 0 else mod(me - 1 + a)

    def wait_block(b):
        for c in load_block(b):
            c.wait()

    def dh(b, j):
        rows, cols = ds(b, R), ds(j, W)
        d = nt(dy_v[rows, :], dwd[cols, :])
        g = dgu[0, rows, cols].astype(F32)
        u = dgu[1, rows, cols].astype(F32)
        g2 = g * g
        t = jnp.tanh(ROOT * (g + CUBE * (g2 * g)))
        cdf = 0.5 * (1.0 + t)
        act = g * cdf
        slope = cdf + g * (0.5 * (1.0 - t * t)) * (ROOT * (1.0 + (3.0 * CUBE) * g2))
        hid[rows, cols] = (act * u).astype(BF)
        dgu[0, rows, cols] = (d * u * slope).astype(BF)
        dgu[1, rows, cols] = (d * act).astype(BF)

    def term(d, s, j):
        rows, tile = ds(rs_block(d, s), R), ds(d * C + j, W)
        return nt(dgu[0, rows, :], dwg[tile, :]) + nt(dgu[1, rows, :], dwu[tile, :])

    def rs_slot(s, j, first=False, last=False, blocks=()):
        if first:
            for d in (0, 1):
                for c in load_w(d * C + j):
                    c.wait()
                buf[d, s, j] = term(d, s, j).astype(BF)
                send(d, s, j, rs(d, s, j))
        else:
            for d in (0, 1):
                rs(d, s - 1, j).wait_recv()
                taken(d)
        if blocks:
            @pl.when(j == 0)
            def _():
                for b in blocks:
                    wait_block(b)
        if not first:
            sums = [buf[d, s, j].astype(F32) + term(d, s, j) for d in (0, 1)]
            for d in (0, 1):
                buf[d, s, j] = sums[d].astype(BF)
            for d in (0, 1):
                if last:
                    send(d, s, j, ag_first(d, j))

                    @pl.when(j > 0)
                    def _():
                        ag_own(d, j - 1).wait()
                    ag_own(d, j).start()
                else:
                    send(d, s, j, rs(d, s, j))
        for b in blocks:
            dh(b, j)

    order = [mod(me - 1), mod(me - 2), me, mod(me - 3), mod(me + 1), mod(me - 4), mod(me + 2), mod(me + 3)]

    def start(copies):
        for c in copies:
            c.start()

    def start_w(j):
        for d in (0, 1):
            start(load_w(d * C + j))

    start(load_block(order[0]))
    start([load_wd(j) for j in range(FT)])
    start_w(0)

    barrier = pltpu.get_barrier_semaphore()
    for p in (left, right):
        pl.semaphore_signal(barrier, inc=1, device_id={"tp": p}, device_id_type=MESH)

    wait_block(order[0])

    for group in (range(0, 2), range(2, FT)):
        for j in group:
            load_wd(j).wait()
        for j in group:
            if j + 1 < C:
                start_w(j + 1)
            if j < 2:
                start(load_block(order[j + 1]))
        for j in group:
            dh(order[0], j)
    pl.semaphore_wait(barrier, 2)

    @pl.loop(0, C)
    def _(j):
        for k in range(5):
            @pl.when(j == k)
            def _():
                start(load_block(order[k + 3]))
        rs_slot(0, j, first=True, blocks=(mod(me - 2), me))

    @pl.loop(0, 2 * C)
    def _(q):
        s, j = q // C + 1, lax.rem(q, C)
        rs_slot(s, j, blocks=(mod(me - 2 - s), mod(me + s)))

    @pl.loop(0, C)
    def _(j):
        rs_slot(3, j, blocks=(mod(me + 3),))

    @pl.loop(0, (n - 5) * C)
    def _(q):
        rs_slot(q // C + 4, lax.rem(q, C))

    for k in (0, 1):
        load_x(k, k).start()

    @pl.loop(0, C)
    def _(j):
        rs_slot(n - 1, j, last=True)

    def forward(q):
        a, j = q // C, lax.rem(q, C)
        for d in (0, 1):
            b = ag_in(d, a)

            @pl.when(a < n - 3)
            def _():
                ag(d, a, j, b).wait_recv()

            @pl.when(a == n - 3)
            def _():
                ag_end(d, j, b).wait_recv()

            @pl.when(a < n - 4)
            def _():
                taken(d)
                send(d, a + n, j, ag(d, a + 1, j, b))

            @pl.when(a == n - 4)
            def _():
                send(d, 2 * n - 4, j, ag_end(d, j, b))

    @pl.loop(0, D // W)
    def _(i):
        k = lax.rem(i, 2)
        load_x(i, k).wait()
        for h, out in ((0, dwg), (1, dwu)):
            out[ds(i, W), :] = tn(xt[k], dgu[h]).astype(BF)
            forward(2 * i + h)

        @pl.when(i + 2 < D // W)
        def _():
            load_x(i + 2, k).start()

    @pl.loop(0, FT)
    def _(i):
        for h in (0, 1):
            dwd[ds(i, W), h * H:(h + 1) * H] = tn(hid[:, ds(i, W)], dy_v[:, h * H:(h + 1) * H]).astype(BF)
            forward(2 * (D // W) + 2 * i + h)

    @pl.loop(0, C)
    def _(j):
        for d in (0, 1):
            for g in (2 * n - 5, 2 * n - 4):
                hop(d, g, j, buf.at[d, 0, j], buf.at[d, 0, j]).wait_send()

    for d in (0, 1):
        ag_own(d, C - 1).wait()


def half(ref, b, R, d):
    H = ref.shape[1] // 2
    return ref.at[pl.ds(pl.multiple_of(b * R, R), R), d * H:(d + 1) * H]


def copy_kernel(n, dx, end_r, end_l, dwg, dwu, dwd, dx_o, dwg_o, dwu_o, dwd_o, stage, in_sem, out_sem, w_sem):
    R = dx.shape[0] // n
    me = lax.axis_index("tp")
    parts = []
    for d, end in ((0, end_r), (1, end_l)):
        for a in range(-1, n - 2):
            b = lax.rem((me - 1 - a if d == 0 else me - 1 + a) + 2 * n, n)
            if d == 1 and a == -1:
                b = lax.rem(me - 2 + n, n)
            src = end if a == n - 3 else half(dx, b, R, d)
            i = len(parts)
            parts.append((pltpu.make_async_copy(src, stage.at[i], in_sem.at[i]),
                          pltpu.make_async_copy(stage.at[i], half(dx_o, b, R, d), out_sem.at[i])))
    whole = [pltpu.make_async_copy(v, o, w_sem.at[i])
             for i, (v, o) in enumerate(((dwg, dwg_o), (dwu, dwu_o), (dwd, dwd_o)))]
    for load, _ in parts:
        load.start()
    for c in whole:
        c.start()
    for load, store in parts:
        load.wait()
        store.start()
    for c in whole:
        c.wait()
    for _, store in parts:
        store.wait()


def end_kernel(n, dx, got_r, got_l, dx_o, sem):
    R = dx.shape[0] // n
    me = lax.axis_index("tp")
    copies = [pltpu.make_async_copy(got_r, half(dx_o, lax.rem(me + 1, n), R, 0), sem.at[0]),
              pltpu.make_async_copy(got_l, half(dx_o, lax.rem(me + n - 3, n), R, 1), sem.at[1])]
    for c in copies:
        c.start()
    for c in copies:
        c.wait()


def solution(mesh):
    n = mesh.shape["tp"]

    def step(x, dy, gate, up, w_gate, w_up, w_down):
        T, D = x.shape
        F = gate.shape[1]
        R, C, FT = T // n, D // 2 // W, F // W
        assert C == FT and n == 8
        dma = pltpu.SemaphoreType.DMA
        any_ = pl.BlockSpec(memory_space=pl.ANY)
        vmem = pl.BlockSpec(memory_space=pltpu.VMEM)
        hbm = pl.BlockSpec(memory_space=pltpu.HBM)
        shape = lambda *s: jax.ShapeDtypeStruct(s, BF)
        dws = [shape(D, F), shape(D, F), shape(F, D)]
        dx, end_r, end_l, *dw = pl.pallas_call(
            functools.partial(kernel, n),
            out_shape=[shape(T, D), shape(R, D // 2), shape(R, D // 2)] + [pltpu.VMEM(w.shape, BF) for w in dws],
            in_specs=[any_] * 7,
            out_specs=[any_] * 3 + [vmem] * 3,
            scratch_shapes=[
                pltpu.VMEM((T, D), BF),
                pltpu.VMEM((2, T, F), BF),
                pltpu.VMEM((T, F), BF),
                pltpu.VMEM((2, n, C, R, W), BF),
                pltpu.VMEM((2, T, W), BF),
                dma((2, 2, C)), dma((2, 2, C)), pltpu.SemaphoreType.REGULAR((2,)),
                dma((3, n)), dma((FT,)), dma((2, 2 * C)), dma((2,)), dma((2,)),
            ],
            compiler_params=pltpu.CompilerParams(
                collective_id=0, has_side_effects=True, vmem_limit_bytes=44 << 20),
            name="mlp_bwd",
        )(x, dy, gate, up, w_gate, w_up, w_down)
        ahead = [(i, (i + 1) % n) for i in range(n)]
        back = [(i, (i - 1) % n) for i in range(n)]
        got_r = lax.ppermute(end_r, "tp", ahead)
        got_l = lax.ppermute(end_l, "tp", back)
        m = 2 * (n - 1)
        dx, *dw = pl.pallas_call(
            functools.partial(copy_kernel, n),
            out_shape=[shape(T, D)] + dws,
            in_specs=[hbm] * 3 + [vmem] * 3,
            out_specs=[hbm] * 4,
            scratch_shapes=[pltpu.VMEM((m, R, D // 2), BF), dma((m,)), dma((m,)), dma((3,))],
            compiler_params=pltpu.CompilerParams(vmem_limit_bytes=10 << 20),
            cost_estimate=pl.CostEstimate(flops=13_000_000_000, bytes_accessed=41_000_000, transcendentals=0),
            name="place",
        )(*(pltpu.with_memory_space_constraint(v, pltpu.HBM) for v in (dx, end_r, end_l)), *dw)
        dx = pl.pallas_call(
            functools.partial(end_kernel, n),
            out_shape=shape(T, D),
            in_specs=[any_, vmem, vmem],
            out_specs=any_,
            scratch_shapes=[dma((2,))],
            input_output_aliases={0: 0},
            compiler_params=pltpu.CompilerParams(vmem_limit_bytes=1 << 20),
            name="place_end",
        )(dx, got_r, got_l)
        return dx, *dw

    tokens, columns, rows = P("dp", None), P(None, "tp"), P("tp", None)
    return jax.shard_map(
        step,
        mesh=mesh,
        in_specs=(tokens, tokens, P("dp", "tp"), P("dp", "tp"), columns, columns, rows),
        out_specs=(tokens, P("dp", "tp"), P("dp", "tp"), P(("dp", "tp"), None)),
        check_vma=False,
    )
```

```python
import functools

import jax
import jax.numpy as jnp
from jax import lax
from jax.experimental import pallas as pl
from jax.experimental.pallas import tpu as pltpu
from jax.sharding import PartitionSpec as P

BF = jnp.bfloat16
F32 = jnp.float32
W = 256
MESH = pl.DeviceIdType.MESH
ROOT = 0.7978845608028654
CUBE = 0.044715


def nt(a, b):
    return lax.dot_general(a, b, (((1,), (1,)), ((), ())), preferred_element_type=F32)


def tn(a, b):
    return lax.dot_general(a, b, (((0,), (0,)), ((), ())), preferred_element_type=F32)


def kernel(n, x, dy, gate, up, wg, wu, wd, dx, end_r, end_l, dwg, dwu, dwd,
           dy_v, dgu, hid, buf, xt,
           send_sem, recv_sem, credit, in_sem, wd_sem, w_sem, own_sem, x_sem):
    T, D = x.shape
    F = gate.shape[1]
    R = T // n
    H = D // 2
    C = H // W
    FT = F // W
    me = lax.axis_index("tp")
    right, left = lax.rem(me + 1, n), lax.rem(me + n - 1, n)
    to = (right, left)

    def mod(b):
        return lax.rem(b + 2 * n, n)

    def ds(i, size):
        return pl.ds(pl.multiple_of(i * size, size), size)

    def load_block(b):
        rows = ds(b, R)
        return (pltpu.make_async_copy(dy.at[rows, :], dy_v.at[rows, :], in_sem.at[0, b]),
                pltpu.make_async_copy(gate.at[rows, :], dgu.at[0, rows, :], in_sem.at[1, b]),
                pltpu.make_async_copy(up.at[rows, :], dgu.at[1, rows, :], in_sem.at[2, b]))

    def load_wd(j):
        return pltpu.make_async_copy(wd.at[ds(j, W), :], dwd.at[ds(j, W), :], wd_sem.at[j])

    def load_w(t):
        return (pltpu.make_async_copy(wg.at[ds(t, W), :], dwg.at[ds(t, W), :], w_sem.at[0, t]),
                pltpu.make_async_copy(wu.at[ds(t, W), :], dwu.at[ds(t, W), :], w_sem.at[1, t]))

    def load_x(i, k):
        return pltpu.make_async_copy(x.at[:, ds(i, W)], xt.at[k], x_sem.at[k])

    def hop(d, g, j, src, dst):
        k = lax.rem(g, 2)
        return pltpu.make_async_remote_copy(
            src_ref=src, dst_ref=dst, send_sem=send_sem.at[d, k, j], recv_sem=recv_sem.at[d, k, j],
            device_id={"tp": to[d]}, device_id_type=MESH)

    def rs(d, s, j):
        return hop(d, s, j, buf.at[d, s, j], buf.at[d, s + 1, j])

    def send(d, g, j, copy):
        def ready():
            hop(d, g, j, buf.at[d, 0, j], buf.at[d, 0, j]).wait_send()
            pl.semaphore_wait(credit.at[d], 1)

        if isinstance(g, int):
            if g >= 2:
                ready()
        else:
            pl.when(g >= 2)(ready)
        copy.start()

    def taken(d):
        pl.semaphore_signal(credit.at[d], inc=1, device_id={"tp": to[1 - d]}, device_id_type=MESH)

    def rs_block(d, s):
        return mod(me - 1 - s) if d == 0 else mod(me - 1 + s)

    def piece(d, b, j):
        return dx.at[ds(b, R), ds(d * C + j, W)]

    def ag_first(d, j):
        return hop(d, n - 1, j, buf.at[d, n - 1, j], piece(d, rs_block(d, n - 1), j))

    def ag_own(d, j):
        return pltpu.make_async_copy(buf.at[d, n - 1, j], piece(d, rs_block(d, n - 1), j), own_sem.at[d])

    def ag(d, a, j, b):
        return hop(d, a + n - 1, j, piece(d, b, j), piece(d, b, j))

    def ag_end(d, j, b):
        return hop(d, 2 * n - 4, j, piece(d, b, j), (end_r, end_l)[d].at[:, ds(j, W)])

    def ag_in(d, a):
        return mod(me - 1 - a) if d == 0 else mod(me - 1 + a)

    def wait_block(b):
        for c in load_block(b):
            c.wait()

    def dh(b, j):
        rows, cols = ds(b, R), ds(j, W)
        d = nt(dy_v[rows, :], dwd[cols, :])
        g = dgu[0, rows, cols].astype(F32)
        u = dgu[1, rows, cols].astype(F32)
        g2 = g * g
        t = jnp.tanh(ROOT * (g + CUBE * (g2 * g)))
        cdf = 0.5 * (1.0 + t)
        act = g * cdf
        slope = cdf + g * (0.5 * (1.0 - t * t)) * (ROOT * (1.0 + (3.0 * CUBE) * g2))
        hid[rows, cols] = (act * u).astype(BF)
        dgu[0, rows, cols] = (d * u * slope).astype(BF)
        dgu[1, rows, cols] = (d * act).astype(BF)

    def term(d, s, j):
        rows, tile = ds(rs_block(d, s), R), ds(d * C + j, W)
        return nt(dgu[0, rows, :], dwg[tile, :]) + nt(dgu[1, rows, :], dwu[tile, :])

    def rs_slot(s, j, first=False, last=False, blocks=()):
        if first:
            for d in (0, 1):
                for c in load_w(d * C + j):
                    c.wait()
        else:
            for d in (0, 1):
                rs(d, s - 1, j).wait_recv()
                taken(d)
        if blocks and not first:
            @pl.when(j == 0)
            def _():
                for b in blocks:
                    wait_block(b)
        sums = [term(d, s, j) for d in (0, 1)]
        if not first:
            sums = [buf[d, s, j].astype(F32) + sums[d] for d in (0, 1)]
        for d in (0, 1):
            buf[d, s, j] = sums[d].astype(BF)
        for d in (0, 1):
            if last:
                send(d, s, j, ag_first(d, j))

                @pl.when(j > 0)
                def _():
                    ag_own(d, j - 1).wait()
                ag_own(d, j).start()
            else:
                send(d, s, j, rs(d, s, j))
        if blocks and first:
            @pl.when(j == 0)
            def _():
                for b in blocks:
                    wait_block(b)
        for b in blocks:
            dh(b, j)

    order = [mod(me - 1), mod(me - 2), me, mod(me - 3), mod(me + 1), mod(me - 4), mod(me + 2), mod(me + 3)]

    def start(copies):
        for c in copies:
            c.start()

    def start_w(j):
        for d in (0, 1):
            start(load_w(d * C + j))

    start(load_block(order[0]))
    start([load_wd(j) for j in range(2)])

    barrier = pltpu.get_barrier_semaphore()
    for p in (left, right):
        pl.semaphore_signal(barrier, inc=1, device_id={"tp": p}, device_id_type=MESH)

    wait_block(order[0])
    start([load_wd(j) for j in range(2, FT)])
    start_w(0)
    for b in order[1:3]:
        start(load_block(b))

    for group in (range(0, 2), range(2, FT)):
        for j in group:
            load_wd(j).wait()
        if 2 in group:
            for j in range(1, C):
                start_w(j)
        for j in group:
            dh(order[0], j)
    pl.semaphore_wait(barrier, 2)

    @pl.loop(0, C)
    def _(j):
        for k in range(5):
            @pl.when(j == k)
            def _():
                start(load_block(order[k + 3]))
        rs_slot(0, j, first=True, blocks=(mod(me - 2), me))

    @pl.loop(0, 2 * C)
    def _(q):
        s, j = q // C + 1, lax.rem(q, C)
        rs_slot(s, j, blocks=(mod(me - 2 - s), mod(me + s)))

    @pl.loop(0, C)
    def _(j):
        rs_slot(3, j, blocks=(mod(me + 3),))

    @pl.loop(0, (n - 5) * C)
    def _(q):
        rs_slot(q // C + 4, lax.rem(q, C))

    for k in (0, 1):
        load_x(k, k).start()

    @pl.loop(0, C)
    def _(j):
        rs_slot(n - 1, j, last=True)

    def forward(q):
        a, j = q // C, lax.rem(q, C)
        for d in (0, 1):
            b = ag_in(d, a)

            @pl.when(a < n - 3)
            def _():
                ag(d, a, j, b).wait_recv()

            @pl.when(a == n - 3)
            def _():
                ag_end(d, j, b).wait_recv()

            @pl.when(a < n - 4)
            def _():
                taken(d)
                send(d, a + n, j, ag(d, a + 1, j, b))

            @pl.when(a == n - 4)
            def _():
                send(d, 2 * n - 4, j, ag_end(d, j, b))

    ahead = 2
    for q in range(ahead):
        forward(q)

    @pl.loop(0, D // W)
    def _(i):
        k = lax.rem(i, 2)
        load_x(i, k).wait()
        for h, out in ((0, dwg), (1, dwu)):
            out[ds(i, W), :] = tn(xt[k], dgu[h]).astype(BF)
            forward(2 * i + h + ahead)

        @pl.when(i + 2 < D // W)
        def _():
            load_x(i + 2, k).start()

    @pl.loop(0, FT)
    def _(i):
        for h in (0, 1):
            dwd[ds(i, W), h * H:(h + 1) * H] = tn(hid[:, ds(i, W)], dy_v[:, h * H:(h + 1) * H]).astype(BF)
            q = 2 * (D // W) + 2 * i + h + ahead

            @pl.when(q < (n - 3) * C)
            def _():
                forward(q)

    @pl.loop((n - 3) * C, (n - 2) * C)
    def _(q):
        forward(q)

    @pl.loop(0, C)
    def _(j):
        for d in (0, 1):
            for g in (2 * n - 5, 2 * n - 4):
                hop(d, g, j, buf.at[d, 0, j], buf.at[d, 0, j]).wait_send()

    for d in (0, 1):
        ag_own(d, C - 1).wait()


def half(ref, b, R, d):
    H = ref.shape[1] // 2
    return ref.at[pl.ds(pl.multiple_of(b * R, R), R), d * H:(d + 1) * H]


def copy_kernel(n, dx, end_r, end_l, dwg, dwu, dwd, dx_o, dwg_o, dwu_o, dwd_o, stage, in_sem, out_sem, w_sem):
    R = dx.shape[0] // n
    me = lax.axis_index("tp")
    parts = []
    for d, end in ((0, end_r), (1, end_l)):
        for a in range(-1, n - 2):
            b = lax.rem((me - 1 - a if d == 0 else me - 1 + a) + 2 * n, n)
            if d == 1 and a == -1:
                b = lax.rem(me - 2 + n, n)
            src = end if a == n - 3 else half(dx, b, R, d)
            i = len(parts)
            parts.append((pltpu.make_async_copy(src, stage.at[i], in_sem.at[i]),
                          pltpu.make_async_copy(stage.at[i], half(dx_o, b, R, d), out_sem.at[i])))
    whole = [pltpu.make_async_copy(v, o, w_sem.at[i])
             for i, (v, o) in enumerate(((dwg, dwg_o), (dwu, dwu_o), (dwd, dwd_o)))]
    for load, _ in parts:
        load.start()
    for c in whole:
        c.start()
    for load, store in parts:
        load.wait()
        store.start()
    for c in whole:
        c.wait()
    for _, store in parts:
        store.wait()


def end_kernel(n, dx, got_r, got_l, dx_o, sem):
    R = dx.shape[0] // n
    me = lax.axis_index("tp")
    copies = [pltpu.make_async_copy(got_r, half(dx_o, lax.rem(me + 1, n), R, 0), sem.at[0]),
              pltpu.make_async_copy(got_l, half(dx_o, lax.rem(me + n - 3, n), R, 1), sem.at[1])]
    for c in copies:
        c.start()
    for c in copies:
        c.wait()


def solution(mesh):
    n = mesh.shape["tp"]

    def step(x, dy, gate, up, w_gate, w_up, w_down):
        T, D = x.shape
        F = gate.shape[1]
        R, C, FT = T // n, D // 2 // W, F // W
        assert C == FT and n == 8
        dma = pltpu.SemaphoreType.DMA
        any_ = pl.BlockSpec(memory_space=pl.ANY)
        vmem = pl.BlockSpec(memory_space=pltpu.VMEM)
        hbm = pl.BlockSpec(memory_space=pltpu.HBM)
        shape = lambda *s: jax.ShapeDtypeStruct(s, BF)
        dws = [shape(D, F), shape(D, F), shape(F, D)]
        dx, end_r, end_l, *dw = pl.pallas_call(
            functools.partial(kernel, n),
            out_shape=[shape(T, D), shape(R, D // 2), shape(R, D // 2)] + [pltpu.VMEM(w.shape, BF) for w in dws],
            in_specs=[any_] * 7,
            out_specs=[any_] * 3 + [vmem] * 3,
            scratch_shapes=[
                pltpu.VMEM((T, D), BF),
                pltpu.VMEM((2, T, F), BF),
                pltpu.VMEM((T, F), BF),
                pltpu.VMEM((2, n, C, R, W), BF),
                pltpu.VMEM((2, T, W), BF),
                dma((2, 2, C)), dma((2, 2, C)), pltpu.SemaphoreType.REGULAR((2,)),
                dma((3, n)), dma((FT,)), dma((2, 2 * C)), dma((2,)), dma((2,)),
            ],
            compiler_params=pltpu.CompilerParams(
                collective_id=0, has_side_effects=True, vmem_limit_bytes=44 << 20),
            name="mlp_bwd",
        )(x, dy, gate, up, w_gate, w_up, w_down)
        ahead = [(i, (i + 1) % n) for i in range(n)]
        back = [(i, (i - 1) % n) for i in range(n)]
        got_r = lax.ppermute(end_r, "tp", ahead)
        got_l = lax.ppermute(end_l, "tp", back)
        m = 2 * (n - 1)
        dx, *dw = pl.pallas_call(
            functools.partial(copy_kernel, n),
            out_shape=[shape(T, D)] + dws,
            in_specs=[hbm] * 3 + [vmem] * 3,
            out_specs=[hbm] * 4,
            scratch_shapes=[pltpu.VMEM((m, R, D // 2), BF), dma((m,)), dma((m,)), dma((3,))],
            compiler_params=pltpu.CompilerParams(vmem_limit_bytes=10 << 20),
            cost_estimate=pl.CostEstimate(flops=13_000_000_000, bytes_accessed=41_000_000, transcendentals=0),
            name="place",
        )(*(pltpu.with_memory_space_constraint(v, pltpu.HBM) for v in (dx, end_r, end_l)), *dw)
        dx = pl.pallas_call(
            functools.partial(end_kernel, n),
            out_shape=shape(T, D),
            in_specs=[any_, vmem, vmem],
            out_specs=any_,
            scratch_shapes=[dma((2,))],
            input_output_aliases={0: 0},
            compiler_params=pltpu.CompilerParams(vmem_limit_bytes=1 << 20),
            name="place_end",
        )(dx, got_r, got_l)
        return dx, *dw

    tokens, columns, rows = P("dp", None), P(None, "tp"), P("tp", None)
    return jax.shard_map(
        step,
        mesh=mesh,
        in_specs=(tokens, tokens, P("dp", "tp"), P("dp", "tp"), columns, columns, rows),
        out_specs=(tokens, P("dp", "tp"), P("dp", "tp"), P(("dp", "tp"), None)),
        check_vma=False,
    )
```

```python
import functools

import jax
import jax.numpy as jnp
from jax import lax
from jax.experimental import pallas as pl
from jax.experimental.pallas import tpu as pltpu
from jax.sharding import PartitionSpec as P

BF = jnp.bfloat16
F32 = jnp.float32
W = 256
MESH = pl.DeviceIdType.MESH
ROOT = 0.7978845608028654
CUBE = 0.044715


def nt(a, b):
    return lax.dot_general(a, b, (((1,), (1,)), ((), ())), preferred_element_type=F32)


def tn(a, b):
    return lax.dot_general(a, b, (((0,), (0,)), ((), ())), preferred_element_type=F32)


def kernel(n, x, dy, gate, up, wg, wu, wd, dx, end_r, end_l, dwg, dwu, dwd,
           dy_v, dgu, hid, buf, xt,
           send_sem, recv_sem, credit, in_sem, wd_sem, w_sem, own_sem, x_sem):
    T, D = x.shape
    F = gate.shape[1]
    R = T // n
    H = D // 2
    C = H // W
    FT = F // W
    me = lax.axis_index("tp")
    right, left = lax.rem(me + 1, n), lax.rem(me + n - 1, n)
    to = (right, left)

    def mod(b):
        return lax.rem(b + 2 * n, n)

    def ds(i, size):
        return pl.ds(pl.multiple_of(i * size, size), size)

    def load_block(b):
        rows = ds(b, R)
        return (pltpu.make_async_copy(dy.at[rows, :], dy_v.at[rows, :], in_sem.at[0, b]),
                pltpu.make_async_copy(gate.at[rows, :], dgu.at[0, rows, :], in_sem.at[1, b]),
                pltpu.make_async_copy(up.at[rows, :], dgu.at[1, rows, :], in_sem.at[2, b]))

    def load_wd(j):
        return pltpu.make_async_copy(wd.at[ds(j, W), :], dwd.at[ds(j, W), :], wd_sem.at[j])

    def load_w(t):
        return (pltpu.make_async_copy(wg.at[ds(t, W), :], dwg.at[ds(t, W), :], w_sem.at[0, t]),
                pltpu.make_async_copy(wu.at[ds(t, W), :], dwu.at[ds(t, W), :], w_sem.at[1, t]))

    def load_x(i, k):
        return pltpu.make_async_copy(x.at[:, ds(i, W)], xt.at[k], x_sem.at[k])

    def hop(d, g, j, src, dst):
        k = lax.rem(g, 2)
        return pltpu.make_async_remote_copy(
            src_ref=src, dst_ref=dst, send_sem=send_sem.at[d, k, j], recv_sem=recv_sem.at[d, k, j],
            device_id={"tp": to[d]}, device_id_type=MESH)

    def rs(d, s, j):
        return hop(d, s, j, buf.at[d, s, j], buf.at[d, s + 1, j])

    def send(d, g, j, copy):
        def ready():
            hop(d, g, j, buf.at[d, 0, j], buf.at[d, 0, j]).wait_send()
            pl.semaphore_wait(credit.at[d], 1)

        if isinstance(g, int):
            if g >= 2:
                ready()
        else:
            pl.when(g >= 2)(ready)
        copy.start()

    def taken(d):
        pl.semaphore_signal(credit.at[d], inc=1, device_id={"tp": to[1 - d]}, device_id_type=MESH)

    def rs_block(d, s):
        return mod(me - 1 - s) if d == 0 else mod(me - 1 + s)

    def piece(d, b, j):
        return dx.at[ds(b, R), ds(d * C + j, W)]

    def ag_first(d, j):
        return hop(d, n - 1, j, buf.at[d, n - 1, j], piece(d, rs_block(d, n - 1), j))

    def ag_own(d, j):
        return pltpu.make_async_copy(buf.at[d, n - 1, j], piece(d, rs_block(d, n - 1), j), own_sem.at[d])

    def ag(d, a, j, b):
        return hop(d, a + n - 1, j, piece(d, b, j), piece(d, b, j))

    def ag_end(d, j, b):
        return hop(d, 2 * n - 4, j, piece(d, b, j), (end_r, end_l)[d].at[:, ds(j, W)])

    def ag_in(d, a):
        return mod(me - 1 - a) if d == 0 else mod(me - 1 + a)

    def wait_block(b):
        for c in load_block(b):
            c.wait()

    def dh(b, j):
        rows, cols = ds(b, R), ds(j, W)
        d = nt(dy_v[rows, :], dwd[cols, :])
        g = dgu[0, rows, cols].astype(F32)
        u = dgu[1, rows, cols].astype(F32)
        g2 = g * g
        t = jnp.tanh(ROOT * (g + CUBE * (g2 * g)))
        cdf = 0.5 * (1.0 + t)
        act = g * cdf
        slope = cdf + g * (0.5 * (1.0 - t * t)) * (ROOT * (1.0 + (3.0 * CUBE) * g2))
        hid[rows, cols] = (act * u).astype(BF)
        dgu[0, rows, cols] = (d * u * slope).astype(BF)
        dgu[1, rows, cols] = (d * act).astype(BF)

    def term(d, s, j):
        rows, tile = ds(rs_block(d, s), R), ds(d * C + j, W)
        return nt(dgu[0, rows, :], dwg[tile, :]) + nt(dgu[1, rows, :], dwu[tile, :])

    def rs_slot(s, j, first=False, last=False, blocks=()):
        if first:
            for d in (0, 1):
                for c in load_w(d * C + j):
                    c.wait()
        else:
            for d in (0, 1):
                rs(d, s - 1, j).wait_recv()
                taken(d)
        if blocks and not first:
            @pl.when(j == 0)
            def _():
                for b in blocks:
                    wait_block(b)
        sums = [term(d, s, j) for d in (0, 1)]
        if not first:
            sums = [buf[d, s, j].astype(F32) + sums[d] for d in (0, 1)]
        for d in (0, 1):
            buf[d, s, j] = sums[d].astype(BF)
        for d in (0, 1):
            if last:
                send(d, s, j, ag_first(d, j))

                @pl.when(j > 0)
                def _():
                    ag_own(d, j - 1).wait()
                ag_own(d, j).start()
            else:
                send(d, s, j, rs(d, s, j))
        if blocks and first:
            @pl.when(j == 0)
            def _():
                for b in blocks:
                    wait_block(b)
        for b in blocks:
            dh(b, j)

    order = [mod(me - 1), mod(me - 2), me, mod(me - 3), mod(me + 1), mod(me - 4), mod(me + 2), mod(me + 3)]

    def start(copies):
        for c in copies:
            c.start()

    def start_w(j):
        for d in (0, 1):
            start(load_w(d * C + j))

    start(load_block(order[0]))
    start([load_wd(j) for j in range(2)])

    barrier = pltpu.get_barrier_semaphore()
    for p in (left, right):
        pl.semaphore_signal(barrier, inc=1, device_id={"tp": p}, device_id_type=MESH)

    wait_block(order[0])
    start([load_wd(j) for j in range(2, FT)])

    for group in (range(0, 2), range(2, FT)):
        for j in group:
            load_wd(j).wait()
        if 0 in group:
            start_w(0)
        else:
            for b in order[1:3]:
                start(load_block(b))
        for j in group:
            dh(order[0], j)
    start_w(1)
    pl.semaphore_wait(barrier, 2)

    @pl.loop(0, C)
    def _(j):
        @pl.when(j + 2 < C)
        def _():
            start_w(j + 2)
        for k in range(5):
            @pl.when(j == k)
            def _():
                start(load_block(order[k + 3]))
        rs_slot(0, j, first=True, blocks=(mod(me - 2), me))

    @pl.loop(0, 2 * C)
    def _(q):
        s, j = q // C + 1, lax.rem(q, C)
        rs_slot(s, j, blocks=(mod(me - 2 - s), mod(me + s)))

    @pl.loop(0, C)
    def _(j):
        rs_slot(3, j, blocks=(mod(me + 3),))

    @pl.loop(0, (n - 5) * C)
    def _(q):
        rs_slot(q // C + 4, lax.rem(q, C))

    for k in (0, 1):
        load_x(k, k).start()

    @pl.loop(0, C)
    def _(j):
        rs_slot(n - 1, j, last=True)

    def forward(q):
        a, j = q // C, lax.rem(q, C)
        for d in (0, 1):
            b = ag_in(d, a)

            @pl.when(a < n - 3)
            def _():
                ag(d, a, j, b).wait_recv()

            @pl.when(a == n - 3)
            def _():
                ag_end(d, j, b).wait_recv()

            @pl.when(a < n - 4)
            def _():
                taken(d)
                send(d, a + n, j, ag(d, a + 1, j, b))

            @pl.when(a == n - 4)
            def _():
                send(d, 2 * n - 4, j, ag_end(d, j, b))

    ahead = 2
    for q in range(ahead):
        forward(q)

    @pl.loop(0, D // W)
    def _(i):
        k = lax.rem(i, 2)
        load_x(i, k).wait()
        for h, out in ((0, dwg), (1, dwu)):
            out[ds(i, W), :] = tn(xt[k], dgu[h]).astype(BF)
            forward(2 * i + h + ahead)

        @pl.when(i + 2 < D // W)
        def _():
            load_x(i + 2, k).start()

    @pl.loop(0, FT)
    def _(i):
        for h in (0, 1):
            dwd[ds(i, W), h * H:(h + 1) * H] = tn(hid[:, ds(i, W)], dy_v[:, h * H:(h + 1) * H]).astype(BF)
            q = 2 * (D // W) + 2 * i + h + ahead

            @pl.when(q < (n - 3) * C)
            def _():
                forward(q)

    @pl.loop((n - 3) * C, (n - 2) * C)
    def _(q):
        forward(q)

    @pl.loop(0, C)
    def _(j):
        for d in (0, 1):
            for g in (2 * n - 5, 2 * n - 4):
                hop(d, g, j, buf.at[d, 0, j], buf.at[d, 0, j]).wait_send()

    for d in (0, 1):
        ag_own(d, C - 1).wait()


def half(ref, b, R, d):
    H = ref.shape[1] // 2
    return ref.at[pl.ds(pl.multiple_of(b * R, R), R), d * H:(d + 1) * H]


def copy_kernel(n, dx, end_r, end_l, dwg, dwu, dwd, dx_o, dwg_o, dwu_o, dwd_o, stage, in_sem, out_sem, w_sem):
    R = dx.shape[0] // n
    me = lax.axis_index("tp")
    parts, whole = [], []
    for d, end in ((0, end_r), (1, end_l)):
        for a in range(-1, n - 2):
            b = lax.rem((me - 1 - a if d == 0 else me - 1 + a) + 2 * n, n)
            if d == 1 and a == -1:
                b = lax.rem(me - 2 + n, n)
            if a == n - 3:
                whole.append((end, half(dx_o, b, R, d)))
                continue
            i = len(parts)
            parts.append((pltpu.make_async_copy(half(dx, b, R, d), stage.at[i], in_sem.at[i]),
                          pltpu.make_async_copy(stage.at[i], half(dx_o, b, R, d), out_sem.at[i])))
    whole = [pltpu.make_async_copy(v, o, w_sem.at[i])
             for i, (v, o) in enumerate(whole + [(dwg, dwg_o), (dwu, dwu_o), (dwd, dwd_o)])]
    for load, _ in parts:
        load.start()
    for c in whole:
        c.start()
    for load, store in parts:
        load.wait()
        store.start()
    for c in whole:
        c.wait()
    for _, store in parts:
        store.wait()


def end_kernel(n, dx, got_r, got_l, dx_o, sem):
    R = dx.shape[0] // n
    me = lax.axis_index("tp")
    copies = [pltpu.make_async_copy(got_r, half(dx_o, lax.rem(me + 1, n), R, 0), sem.at[0]),
              pltpu.make_async_copy(got_l, half(dx_o, lax.rem(me + n - 3, n), R, 1), sem.at[1])]
    for c in copies:
        c.start()
    for c in copies:
        c.wait()


def solution(mesh):
    n = mesh.shape["tp"]

    def step(x, dy, gate, up, w_gate, w_up, w_down):
        T, D = x.shape
        F = gate.shape[1]
        R, C, FT = T // n, D // 2 // W, F // W
        assert C == FT and n == 8
        dma = pltpu.SemaphoreType.DMA
        any_ = pl.BlockSpec(memory_space=pl.ANY)
        vmem = pl.BlockSpec(memory_space=pltpu.VMEM)
        hbm = pl.BlockSpec(memory_space=pltpu.HBM)
        shape = lambda *s: jax.ShapeDtypeStruct(s, BF)
        ends = [shape(R, D // 2)] * 2
        dws = [shape(D, F), shape(D, F), shape(F, D)]
        dx, end_r, end_l, *dw = pl.pallas_call(
            functools.partial(kernel, n),
            out_shape=[shape(T, D)] + [pltpu.VMEM(w.shape, BF) for w in ends + dws],
            in_specs=[any_] * 7,
            out_specs=[any_] + [vmem] * 5,
            scratch_shapes=[
                pltpu.VMEM((T, D), BF),
                pltpu.VMEM((2, T, F), BF),
                pltpu.VMEM((T, F), BF),
                pltpu.VMEM((2, n, C, R, W), BF),
                pltpu.VMEM((2, T, W), BF),
                dma((2, 2, C)), dma((2, 2, C)), pltpu.SemaphoreType.REGULAR((2,)),
                dma((3, n)), dma((FT,)), dma((2, 2 * C)), dma((2,)), dma((2,)),
            ],
            compiler_params=pltpu.CompilerParams(
                collective_id=0, has_side_effects=True, vmem_limit_bytes=43 << 20),
            name="mlp_bwd",
        )(x, dy, gate, up, w_gate, w_up, w_down)
        ahead = [(i, (i + 1) % n) for i in range(n)]
        back = [(i, (i - 1) % n) for i in range(n)]
        got_r = lax.ppermute(end_r, "tp", ahead)
        got_l = lax.ppermute(end_l, "tp", back)
        m = 2 * (n - 2)
        dx, *dw = pl.pallas_call(
            functools.partial(copy_kernel, n),
            out_shape=[shape(T, D)] + dws,
            in_specs=[hbm] + [vmem] * 5,
            out_specs=[hbm] * 4,
            scratch_shapes=[pltpu.VMEM((m, R, D // 2), BF), dma((m,)), dma((m,)), dma((5,))],
            compiler_params=pltpu.CompilerParams(vmem_limit_bytes=10 << 20),
            cost_estimate=pl.CostEstimate(flops=13_000_000_000, bytes_accessed=41_000_000, transcendentals=0),
            name="place",
        )(pltpu.with_memory_space_constraint(dx, pltpu.HBM), end_r, end_l, *dw)
        dx = pl.pallas_call(
            functools.partial(end_kernel, n),
            out_shape=shape(T, D),
            in_specs=[any_, vmem, vmem],
            out_specs=any_,
            scratch_shapes=[dma((2,))],
            input_output_aliases={0: 0},
            compiler_params=pltpu.CompilerParams(vmem_limit_bytes=1 << 20),
            name="place_end",
        )(dx, got_r, got_l)
        return dx, *dw

    tokens, columns, rows = P("dp", None), P(None, "tp"), P("tp", None)
    return jax.shard_map(
        step,
        mesh=mesh,
        in_specs=(tokens, tokens, P("dp", "tp"), P("dp", "tp"), columns, columns, rows),
        out_specs=(tokens, P("dp", "tp"), P("dp", "tp"), P(("dp", "tp"), None)),
        check_vma=False,
    )
```

```python
import functools

import jax
import jax.numpy as jnp
from jax import lax
from jax.experimental import pallas as pl
from jax.experimental.pallas import tpu as pltpu
from jax.sharding import PartitionSpec as P

BF = jnp.bfloat16
F32 = jnp.float32
W = 256
MESH = pl.DeviceIdType.MESH
ROOT = 0.7978845608028654
CUBE = 0.044715


def nt(a, b):
    return lax.dot_general(a, b, (((1,), (1,)), ((), ())), preferred_element_type=F32)


def tn(a, b):
    return lax.dot_general(a, b, (((0,), (0,)), ((), ())), preferred_element_type=F32)


def kernel(n, x, dy, gate, up, wg, wu, wd, dx, end_r, end_l, dwg, dwu, dwd,
           dy_v, dgu, hid, buf, xt,
           send_sem, recv_sem, credit, in_sem, wd_sem, w_sem, own_sem, x_sem):
    T, D = x.shape
    F = gate.shape[1]
    R = T // n
    H = D // 2
    C = H // W
    FT = F // W
    me = lax.axis_index("tp")
    right, left = lax.rem(me + 1, n), lax.rem(me + n - 1, n)
    to = (right, left)

    def mod(b):
        return lax.rem(b + 2 * n, n)

    def ds(i, size):
        return pl.ds(pl.multiple_of(i * size, size), size)

    def load_block(b, i):
        rows, k = ds(b, R), lax.rem(i, 6)
        return (pltpu.make_async_copy(dy.at[rows, :], dy_v.at[rows, :], in_sem.at[0, k]),
                pltpu.make_async_copy(gate.at[rows, :], dgu.at[0, rows, :], in_sem.at[1, k]),
                pltpu.make_async_copy(up.at[rows, :], dgu.at[1, rows, :], in_sem.at[2, k]))

    def load_wd(j):
        return pltpu.make_async_copy(wd.at[ds(j, W), :], dwd.at[ds(j, W), :], wd_sem.at[j])

    def load_w(d, j):
        t, k = d * C + j, lax.rem(j, 3)
        return (pltpu.make_async_copy(wg.at[ds(t, W), :], dwg.at[ds(t, W), :], w_sem.at[0, d, k]),
                pltpu.make_async_copy(wu.at[ds(t, W), :], dwu.at[ds(t, W), :], w_sem.at[1, d, k]))

    def load_x(i, k):
        return pltpu.make_async_copy(x.at[:, ds(i, W)], xt.at[k], x_sem.at[k])

    def hop(d, g, j, src, dst):
        k = lax.rem(g, 2)
        return pltpu.make_async_remote_copy(
            src_ref=src, dst_ref=dst, send_sem=send_sem.at[d, k, j], recv_sem=recv_sem.at[d, k, j],
            device_id={"tp": to[d]}, device_id_type=MESH)

    def rs(d, s, j):
        return hop(d, s, j, buf.at[d, s, j], buf.at[d, s + 1, j])

    def send(d, g, j, copy):
        def ready():
            hop(d, g, j, buf.at[d, 0, j], buf.at[d, 0, j]).wait_send()
            pl.semaphore_wait(credit.at[d], 1)

        if isinstance(g, int):
            if g >= 2:
                ready()
        else:
            pl.when(g >= 2)(ready)
        copy.start()

    def taken(d):
        pl.semaphore_signal(credit.at[d], inc=1, device_id={"tp": to[1 - d]}, device_id_type=MESH)

    def rs_block(d, s):
        return mod(me - 1 - s) if d == 0 else mod(me - 1 + s)

    def piece(d, b, j):
        return dx.at[ds(b, R), ds(d * C + j, W)]

    def ag_first(d, j):
        return hop(d, n - 1, j, buf.at[d, n - 1, j], piece(d, rs_block(d, n - 1), j))

    def ag_own(d, j):
        return pltpu.make_async_copy(buf.at[d, n - 1, j], piece(d, rs_block(d, n - 1), j), own_sem.at[d])

    def ag(d, a, j, b):
        return hop(d, a + n - 1, j, piece(d, b, j), piece(d, b, j))

    def ag_end(d, j, b):
        return hop(d, 2 * n - 4, j, piece(d, b, j), (end_r, end_l)[d].at[:, ds(j, W)])

    def ag_in(d, a):
        return mod(me - 1 - a) if d == 0 else mod(me - 1 + a)

    def wait_block(b, i):
        for c in load_block(b, i):
            c.wait()

    def dh(b, j):
        rows, cols = ds(b, R), ds(j, W)
        d = nt(dy_v[rows, :], dwd[cols, :])
        g = dgu[0, rows, cols].astype(F32)
        u = dgu[1, rows, cols].astype(F32)
        g2 = g * g
        t = jnp.tanh(g * (ROOT + (ROOT * CUBE) * g2))
        cdf = 0.5 + 0.5 * t
        act = g * cdf
        slope = cdf + (act * (1.0 - t)) * (ROOT + (3.0 * ROOT * CUBE) * g2)
        hid[rows, cols] = (act * u).astype(BF)
        dgu[0, rows, cols] = (d * u * slope).astype(BF)
        dgu[1, rows, cols] = (d * act).astype(BF)

    def term(d, s, j):
        rows, tile = ds(rs_block(d, s), R), ds(d * C + j, W)
        return nt(dgu[0, rows, :], dwg[tile, :]) + nt(dgu[1, rows, :], dwu[tile, :])

    def rs_slot(s, j, first=False, last=False, blocks=()):
        if first:
            for d in (0, 1):
                for c in load_w(d, j):
                    c.wait()
        else:
            for d in (0, 1):
                rs(d, s - 1, j).wait_recv()
                taken(d)
        if blocks and not first:
            @pl.when(j == 0)
            def _():
                for i, b in enumerate(blocks):
                    wait_block(b, 2 * s + 1 + i)
        sums = [term(d, s, j) for d in (0, 1)]
        if not first:
            sums = [buf[d, s, j].astype(F32) + sums[d] for d in (0, 1)]
        for d in (0, 1):
            buf[d, s, j] = sums[d].astype(BF)
        for d in (0, 1):
            if last:
                send(d, s, j, ag_first(d, j))

                @pl.when(j > 0)
                def _():
                    ag_own(d, j - 1).wait()
                ag_own(d, j).start()
            else:
                send(d, s, j, rs(d, s, j))
        if blocks and first:
            @pl.when(j == 0)
            def _():
                for i, b in enumerate(blocks):
                    wait_block(b, 2 * s + 1 + i)
        for b in blocks:
            dh(b, j)

    order = [mod(me - 1), mod(me - 2), me, mod(me - 3), mod(me + 1), mod(me - 4), mod(me + 2), mod(me + 3)]

    def start(copies):
        for c in copies:
            c.start()

    def start_w(j):
        for d in (0, 1):
            start(load_w(d, j))

    start(load_block(order[0], 0))
    start([load_wd(j) for j in range(3)])

    barrier = pltpu.get_barrier_semaphore()
    for p in (left, right):
        pl.semaphore_signal(barrier, inc=1, device_id={"tp": p}, device_id_type=MESH)

    wait_block(order[0], 0)
    start([load_wd(j) for j in range(3, FT)])

    for group in (range(0, 3), range(3, FT)):
        for j in group:
            load_wd(j).wait()
        if 0 in group:
            start_w(0)
        else:
            for i in (1, 2):
                start(load_block(order[i], i))
        for j in group:
            dh(order[0], j)
    start_w(1)
    pl.semaphore_wait(barrier, 2)

    @pl.loop(0, C)
    def _(j):
        @pl.when(j + 2 < C)
        def _():
            start_w(j + 2)
        for k in range(5):
            @pl.when(j == k)
            def _():
                start(load_block(order[k + 3], k + 3))
        rs_slot(0, j, first=True, blocks=(mod(me - 2), me))

    @pl.loop(0, 2 * C)
    def _(q):
        s, j = q // C + 1, lax.rem(q, C)
        rs_slot(s, j, blocks=(mod(me - 2 - s), mod(me + s)))

    @pl.loop(0, C)
    def _(j):
        rs_slot(3, j, blocks=(mod(me + 3),))

    @pl.loop(0, (n - 5) * C)
    def _(q):
        rs_slot(q // C + 4, lax.rem(q, C))

    for k in (0, 1):
        load_x(k, k).start()

    @pl.loop(0, C)
    def _(j):
        rs_slot(n - 1, j, last=True)

    def forward(q):
        a, j = q // C, lax.rem(q, C)
        for d in (0, 1):
            b = ag_in(d, a)

            @pl.when(a < n - 3)
            def _():
                ag(d, a, j, b).wait_recv()

            @pl.when(a == n - 3)
            def _():
                ag_end(d, j, b).wait_recv()

            @pl.when(a < n - 4)
            def _():
                taken(d)
                send(d, a + n, j, ag(d, a + 1, j, b))

            @pl.when(a == n - 4)
            def _():
                send(d, 2 * n - 4, j, ag_end(d, j, b))

    ahead = 2
    for q in range(ahead):
        forward(q)

    @pl.loop(0, D // W)
    def _(i):
        k = lax.rem(i, 2)
        load_x(i, k).wait()
        for h, out in ((0, dwg), (1, dwu)):
            out[ds(i, W), :] = tn(xt[k], dgu[h]).astype(BF)
            forward(2 * i + h + ahead)

        @pl.when(i + 2 < D // W)
        def _():
            load_x(i + 2, k).start()

    @pl.loop(0, FT)
    def _(i):
        for h in (0, 1):
            dwd[ds(i, W), h * H:(h + 1) * H] = tn(hid[:, ds(i, W)], dy_v[:, h * H:(h + 1) * H]).astype(BF)
            q = 2 * (D // W) + 2 * i + h + ahead

            @pl.when(q < (n - 3) * C)
            def _():
                forward(q)

    @pl.loop((n - 3) * C, (n - 2) * C)
    def _(q):
        forward(q)

    @pl.loop(0, C)
    def _(j):
        for d in (0, 1):
            for g in (2 * n - 5, 2 * n - 4):
                hop(d, g, j, buf.at[d, 0, j], buf.at[d, 0, j]).wait_send()

    for d in (0, 1):
        ag_own(d, C - 1).wait()


def half(ref, b, R, d):
    H = ref.shape[1] // 2
    return ref.at[pl.ds(pl.multiple_of(b * R, R), R), d * H:(d + 1) * H]


def copy_kernel(n, dx, end_r, end_l, dwg, dwu, dwd, dx_o, dwg_o, dwu_o, dwd_o, stage, in_sem, out_sem, w_sem):
    R = dx.shape[0] // n
    me = lax.axis_index("tp")
    parts, whole = [], []
    for d, end in ((0, end_r), (1, end_l)):
        for a in range(-1, n - 2):
            b = lax.rem((me - 1 - a if d == 0 else me - 1 + a) + 2 * n, n)
            if d == 1 and a == -1:
                b = lax.rem(me - 2 + n, n)
            if a == n - 3:
                whole.append((end, half(dx_o, b, R, d)))
                continue
            i = len(parts)
            parts.append((pltpu.make_async_copy(half(dx, b, R, d), stage.at[i], in_sem.at[i]),
                          pltpu.make_async_copy(stage.at[i], half(dx_o, b, R, d), out_sem.at[i])))
    whole = [pltpu.make_async_copy(v, o, w_sem.at[i])
             for i, (v, o) in enumerate(whole + [(dwg, dwg_o), (dwu, dwu_o), (dwd, dwd_o)])]
    for load, _ in parts:
        load.start()
    for c in whole:
        c.start()
    for load, store in parts:
        load.wait()
        store.start()
    for c in whole:
        c.wait()
    for _, store in parts:
        store.wait()


def end_kernel(n, dx, got_r, got_l, dx_o, sem):
    R = dx.shape[0] // n
    me = lax.axis_index("tp")
    copies = []
    for d, got, b in ((0, got_r, lax.rem(me + 1, n)), (1, got_l, lax.rem(me + n - 3, n))):
        for i in range(4):
            rows = pl.ds(i * R // 4, R // 4)
            copies.append(pltpu.make_async_copy(got.at[rows, :], half(dx_o, b, R, d).at[rows, :], sem.at[d, i]))
    for c in copies:
        c.start()
    for c in copies:
        c.wait()


def solution(mesh):
    n = mesh.shape["tp"]

    def step(x, dy, gate, up, w_gate, w_up, w_down):
        T, D = x.shape
        F = gate.shape[1]
        R, C, FT = T // n, D // 2 // W, F // W
        assert C == FT and n == 8
        dma = pltpu.SemaphoreType.DMA
        any_ = pl.BlockSpec(memory_space=pl.ANY)
        vmem = pl.BlockSpec(memory_space=pltpu.VMEM)
        hbm = pl.BlockSpec(memory_space=pltpu.HBM)
        shape = lambda *s: jax.ShapeDtypeStruct(s, BF)
        ends = [shape(R, D // 2)] * 2
        dws = [shape(D, F), shape(D, F), shape(F, D)]
        dx, end_r, end_l, *dw = pl.pallas_call(
            functools.partial(kernel, n),
            out_shape=[shape(T, D)] + [pltpu.VMEM(w.shape, BF) for w in ends + dws],
            in_specs=[any_] * 7,
            out_specs=[any_] + [vmem] * 5,
            scratch_shapes=[
                pltpu.VMEM((T, D), BF),
                pltpu.VMEM((2, T, F), BF),
                pltpu.VMEM((T, F), BF),
                pltpu.VMEM((2, n, C, R, W), BF),
                pltpu.VMEM((2, T, W), BF),
                dma((2, 2, C)), dma((2, 2, C)), pltpu.SemaphoreType.REGULAR((2,)),
                dma((3, 6)), dma((FT,)), dma((2, 2, 3)), dma((2,)), dma((2,)),
            ],
            compiler_params=pltpu.CompilerParams(
                collective_id=0, has_side_effects=True, vmem_limit_bytes=43 << 20),
            name="mlp_bwd",
        )(x, dy, gate, up, w_gate, w_up, w_down)
        ahead = [(i, (i + 1) % n) for i in range(n)]
        back = [(i, (i - 1) % n) for i in range(n)]
        got_r = lax.ppermute(end_r, "tp", ahead)
        got_l = lax.ppermute(end_l, "tp", back)
        m = 2 * (n - 2)
        dx, *dw = pl.pallas_call(
            functools.partial(copy_kernel, n),
            out_shape=[shape(T, D)] + dws,
            in_specs=[hbm] + [vmem] * 5,
            out_specs=[hbm] * 4,
            scratch_shapes=[pltpu.VMEM((m, R, D // 2), BF), dma((m,)), dma((m,)), dma((5,))],
            compiler_params=pltpu.CompilerParams(vmem_limit_bytes=10 << 20),
            cost_estimate=pl.CostEstimate(flops=13_000_000_000, bytes_accessed=41_000_000, transcendentals=0),
            name="place",
        )(pltpu.with_memory_space_constraint(dx, pltpu.HBM), end_r, end_l, *dw)
        dx = pl.pallas_call(
            functools.partial(end_kernel, n),
            out_shape=shape(T, D),
            in_specs=[any_, vmem, vmem],
            out_specs=any_,
            scratch_shapes=[dma((2, 4))],
            input_output_aliases={0: 0},
            compiler_params=pltpu.CompilerParams(vmem_limit_bytes=1 << 20),
            name="place_end",
        )(dx, got_r, got_l)
        return dx, *dw

    tokens, columns, rows = P("dp", None), P(None, "tp"), P("tp", None)
    return jax.shard_map(
        step,
        mesh=mesh,
        in_specs=(tokens, tokens, P("dp", "tp"), P("dp", "tp"), columns, columns, rows),
        out_specs=(tokens, P("dp", "tp"), P("dp", "tp"), P(("dp", "tp"), None)),
        check_vma=False,
    )
```

```python
import functools

import jax
import jax.numpy as jnp
from jax import lax
from jax.experimental import pallas as pl
from jax.experimental.pallas import tpu as pltpu
from jax.sharding import PartitionSpec as P

BF = jnp.bfloat16
F32 = jnp.float32
W = 256
MESH = pl.DeviceIdType.MESH
ROOT = 0.7978845608028654
CUBE = 0.044715


def nt(a, b):
    return lax.dot_general(a, b, (((1,), (1,)), ((), ())), preferred_element_type=F32)


def tn(a, b):
    return lax.dot_general(a, b, (((0,), (0,)), ((), ())), preferred_element_type=F32)


def kernel(n, x, dy, gate, up, wg, wu, wd, dx, end_r, end_l, dwg, dwu, dwd,
           dy_v, dgu, hid, buf, xt,
           send_sem, recv_sem, credit, in_sem, wd_sem, w_sem, own_sem, x_sem):
    T, D = x.shape
    F = gate.shape[1]
    R = T // n
    H = D // 2
    C = H // W
    FT = F // W
    me = lax.axis_index("tp")
    right, left = lax.rem(me + 1, n), lax.rem(me + n - 1, n)
    to = (right, left)

    def mod(b):
        return lax.rem(b + 2 * n, n)

    def ds(i, size):
        return pl.ds(pl.multiple_of(i * size, size), size)

    def load_block(b, i):
        rows, k = ds(b, R), lax.rem(i, 6)
        return (pltpu.make_async_copy(dy.at[rows, :], dy_v.at[rows, :], in_sem.at[0, k]),
                pltpu.make_async_copy(gate.at[rows, :], dgu.at[0, rows, :], in_sem.at[1, k]),
                pltpu.make_async_copy(up.at[rows, :], dgu.at[1, rows, :], in_sem.at[2, k]))

    def load_wd(j):
        return pltpu.make_async_copy(wd.at[ds(j, W), :], dwd.at[ds(j, W), :], wd_sem.at[j])

    def load_w(d, j):
        t, k = d * C + j, lax.rem(j, 3)
        return (pltpu.make_async_copy(wg.at[ds(t, W), :], dwg.at[ds(t, W), :], w_sem.at[0, d, k]),
                pltpu.make_async_copy(wu.at[ds(t, W), :], dwu.at[ds(t, W), :], w_sem.at[1, d, k]))

    def load_x(i, k):
        return pltpu.make_async_copy(x.at[:, ds(i, W)], xt.at[k], x_sem.at[k])

    def hop(d, g, j, src, dst):
        k = lax.rem(g, 2)
        return pltpu.make_async_remote_copy(
            src_ref=src, dst_ref=dst, send_sem=send_sem.at[d, k, j], recv_sem=recv_sem.at[d, k, j],
            device_id={"tp": to[d]}, device_id_type=MESH)

    def rs(d, s, j):
        return hop(d, s, j, buf.at[d, s, j], buf.at[d, s + 1, j])

    def send(d, g, j, copy):
        def ready():
            hop(d, g, j, buf.at[d, 0, j], buf.at[d, 0, j]).wait_send()
            pl.semaphore_wait(credit.at[d], 1)

        if isinstance(g, int):
            if g >= 2:
                ready()
        else:
            pl.when(g >= 2)(ready)
        copy.start()

    def taken(d):
        pl.semaphore_signal(credit.at[d], inc=1, device_id={"tp": to[1 - d]}, device_id_type=MESH)

    def rs_block(d, s):
        return mod(me - 1 - s) if d == 0 else mod(me - 1 + s)

    def piece(d, b, j):
        return dx.at[ds(b, R), ds(d * C + j, W)]

    def ag_first(d, j):
        return hop(d, n - 1, j, buf.at[d, n - 1, j], piece(d, rs_block(d, n - 1), j))

    def ag_own(d, j):
        return pltpu.make_async_copy(buf.at[d, n - 1, j], piece(d, rs_block(d, n - 1), j), own_sem.at[d])

    def ag(d, a, j, b):
        return hop(d, a + n - 1, j, piece(d, b, j), piece(d, b, j))

    def ag_end(d, j, b):
        return hop(d, 2 * n - 4, j, piece(d, b, j), (end_r, end_l)[d].at[:, ds(j, W)])

    def ag_in(d, a):
        return mod(me - 1 - a) if d == 0 else mod(me - 1 + a)

    def wait_block(b, i):
        for c in load_block(b, i):
            c.wait()

    def dh(b, j):
        rows, cols = ds(b, R), ds(j, W)
        d = nt(dy_v[rows, :], dwd[cols, :])
        g = dgu[0, rows, cols].astype(F32)
        u = dgu[1, rows, cols].astype(F32)
        g2 = g * g
        t = jnp.tanh(g * (ROOT + (ROOT * CUBE) * g2))
        cdf = 0.5 + 0.5 * t
        act = g * cdf
        slope = cdf + (act * (1.0 - t)) * (ROOT + (3.0 * ROOT * CUBE) * g2)
        hid[rows, cols] = (act * u).astype(BF)
        dgu[0, rows, cols] = (d * u * slope).astype(BF)
        dgu[1, rows, cols] = (d * act).astype(BF)

    def term(d, s, j):
        rows, tile = ds(rs_block(d, s), R), ds(d * C + j, W)
        return nt(dgu[0, rows, :], dwg[tile, :]) + nt(dgu[1, rows, :], dwu[tile, :])

    def rs_slot(s, j, first=False, last=False, blocks=()):
        if first:
            for d in (0, 1):
                for c in load_w(d, j):
                    c.wait()
        else:
            for d in (0, 1):
                rs(d, s - 1, j).wait_recv()
                taken(d)
        if blocks and not first:
            @pl.when(j == 0)
            def _():
                for i, b in enumerate(blocks):
                    wait_block(b, 2 * s + 1 + i)
        sums = [term(d, s, j) for d in (0, 1)]
        if not first:
            sums = [buf[d, s, j].astype(F32) + sums[d] for d in (0, 1)]
        for d in (0, 1):
            buf[d, s, j] = sums[d].astype(BF)
        for d in (0, 1):
            if last:
                send(d, s, j, ag_first(d, j))

                @pl.when(j > 0)
                def _():
                    ag_own(d, j - 1).wait()
                ag_own(d, j).start()
            else:
                send(d, s, j, rs(d, s, j))
        if blocks and first:
            @pl.when(j == 0)
            def _():
                for i, b in enumerate(blocks):
                    wait_block(b, 2 * s + 1 + i)
        for b in blocks:
            dh(b, j)

    order = [mod(me - 1), mod(me - 2), me, mod(me - 3), mod(me + 1), mod(me - 4), mod(me + 2), mod(me + 3)]

    def start(copies):
        for c in copies:
            c.start()

    def start_w(j):
        for d in (0, 1):
            start(load_w(d, j))

    start(load_block(order[0], 0))
    start([load_wd(j) for j in range(3)])

    barrier = pltpu.get_barrier_semaphore()
    for p in (left, right):
        pl.semaphore_signal(barrier, inc=1, device_id={"tp": p}, device_id_type=MESH)

    wait_block(order[0], 0)
    start([load_wd(j) for j in range(3, FT)])

    for group in (range(0, 3), range(3, FT)):
        for j in group:
            load_wd(j).wait()
        if 0 in group:
            start_w(0)
        else:
            for i in (1, 2):
                start(load_block(order[i], i))
        for j in group:
            dh(order[0], j)
    start_w(1)
    pl.semaphore_wait(barrier, 2)

    @pl.loop(0, C)
    def _(j):
        @pl.when(j + 2 < C)
        def _():
            start_w(j + 2)
        for k in range(5):
            @pl.when(j == k)
            def _():
                start(load_block(order[k + 3], k + 3))
        rs_slot(0, j, first=True, blocks=(mod(me - 2), me))

    @pl.loop(0, 2 * C)
    def _(q):
        s, j = q // C + 1, lax.rem(q, C)
        rs_slot(s, j, blocks=(mod(me - 2 - s), mod(me + s)))

    @pl.loop(0, C)
    def _(j):
        rs_slot(3, j, blocks=(mod(me + 3),))

    @pl.loop(0, (n - 5) * C)
    def _(q):
        rs_slot(q // C + 4, lax.rem(q, C))

    for k in (0, 1):
        load_x(k, k).start()

    @pl.loop(0, C)
    def _(j):
        rs_slot(n - 1, j, last=True)

    def forward(q):
        a, j = q // C, lax.rem(q, C)
        for d in (0, 1):
            b = ag_in(d, a)

            @pl.when(a < n - 3)
            def _():
                ag(d, a, j, b).wait_recv()

            @pl.when(a == n - 3)
            def _():
                ag_end(d, j, b).wait_recv()

            @pl.when(a < n - 4)
            def _():
                taken(d)
                send(d, a + n, j, ag(d, a + 1, j, b))

            @pl.when(a == n - 4)
            def _():
                send(d, 2 * n - 4, j, ag_end(d, j, b))

    ahead = 2
    for q in range(ahead):
        forward(q)

    @pl.loop(0, D // W)
    def _(i):
        k = lax.rem(i, 2)
        load_x(i, k).wait()
        for h, out in ((0, dwg), (1, dwu)):
            out[ds(i, W), :] = tn(xt[k], dgu[h]).astype(BF)
            forward(2 * i + h + ahead)

        @pl.when(i + 2 < D // W)
        def _():
            load_x(i + 2, k).start()

    @pl.loop(0, FT)
    def _(i):
        for h in (0, 1):
            dwd[ds(i, W), h * H:(h + 1) * H] = tn(hid[:, ds(i, W)], dy_v[:, h * H:(h + 1) * H]).astype(BF)
            q = 2 * (D // W) + 2 * i + h + ahead

            @pl.when(q < (n - 3) * C)
            def _():
                forward(q)

    @pl.loop((n - 3) * C, (n - 2) * C)
    def _(q):
        forward(q)

    @pl.loop(0, C)
    def _(j):
        for d in (0, 1):
            for g in (2 * n - 5, 2 * n - 4):
                hop(d, g, j, buf.at[d, 0, j], buf.at[d, 0, j]).wait_send()

    for d in (0, 1):
        ag_own(d, C - 1).wait()


def half(ref, b, R, d):
    H = ref.shape[1] // 2
    return ref.at[pl.ds(pl.multiple_of(b * R, R), R), d * H:(d + 1) * H]


def copy_kernel(n, dx, end_r, end_l, dwg, dwu, dwd, dx_o, dwg_o, dwu_o, dwd_o, stage, in_sem, out_sem, w_sem):
    R = dx.shape[0] // n
    me = lax.axis_index("tp")
    parts, whole = [], []
    for d, end in ((0, end_r), (1, end_l)):
        for a in range(-1, n - 2):
            b = lax.rem((me - 1 - a if d == 0 else me - 1 + a) + 2 * n, n)
            if d == 1 and a == -1:
                b = lax.rem(me - 2 + n, n)
            if a == n - 3:
                whole.append((end, half(dx_o, b, R, d)))
                continue
            i = len(parts)
            parts.append((pltpu.make_async_copy(half(dx, b, R, d), stage.at[i], in_sem.at[i]),
                          pltpu.make_async_copy(stage.at[i], half(dx_o, b, R, d), out_sem.at[i])))
    whole = [pltpu.make_async_copy(v, o, w_sem.at[i])
             for i, (v, o) in enumerate(whole + [(dwg, dwg_o), (dwu, dwu_o), (dwd, dwd_o)])]
    for load, _ in parts:
        load.start()
    for c in whole:
        c.start()
    for load, store in parts:
        load.wait()
        store.start()
    for c in whole:
        c.wait()
    for _, store in parts:
        store.wait()


def end_kernel(n, dx, got_r, got_l, dx_o, sem):
    R = dx.shape[0] // n
    me = lax.axis_index("tp")
    copies = []
    for d, got, b in ((0, got_r, lax.rem(me + 1, n)), (1, got_l, lax.rem(me + n - 3, n))):
        for i in range(1):
            rows = pl.ds(i * R, R)
            copies.append(pltpu.make_async_copy(got.at[rows, :], half(dx_o, b, R, d).at[rows, :], sem.at[d, i]))
    for c in copies:
        c.start()
    for c in copies:
        c.wait()


def solution(mesh):
    n = mesh.shape["tp"]

    def step(x, dy, gate, up, w_gate, w_up, w_down):
        T, D = x.shape
        F = gate.shape[1]
        R, C, FT = T // n, D // 2 // W, F // W
        assert C == FT and n == 8
        dma = pltpu.SemaphoreType.DMA
        any_ = pl.BlockSpec(memory_space=pl.ANY)
        vmem = pl.BlockSpec(memory_space=pltpu.VMEM)
        hbm = pl.BlockSpec(memory_space=pltpu.HBM)
        shape = lambda *s: jax.ShapeDtypeStruct(s, BF)
        ends = [shape(R, D // 2)] * 2
        dws = [shape(D, F), shape(D, F), shape(F, D)]
        dx, end_r, end_l, *dw = pl.pallas_call(
            functools.partial(kernel, n),
            out_shape=[shape(T, D)] + [pltpu.VMEM(w.shape, BF) for w in ends + dws],
            in_specs=[any_] * 7,
            out_specs=[any_] + [vmem] * 5,
            scratch_shapes=[
                pltpu.VMEM((T, D), BF),
                pltpu.VMEM((2, T, F), BF),
                pltpu.VMEM((T, F), BF),
                pltpu.VMEM((2, n, C, R, W), BF),
                pltpu.VMEM((2, T, W), BF),
                dma((2, 2, C)), dma((2, 2, C)), pltpu.SemaphoreType.REGULAR((2,)),
                dma((3, 6)), dma((FT,)), dma((2, 2, 3)), dma((2,)), dma((2,)),
            ],
            compiler_params=pltpu.CompilerParams(
                collective_id=0, has_side_effects=True, vmem_limit_bytes=43 << 20),
            name="mlp_bwd",
        )(x, dy, gate, up, w_gate, w_up, w_down)
        ahead = [(i, (i + 1) % n) for i in range(n)]
        back = [(i, (i - 1) % n) for i in range(n)]
        got_r = lax.ppermute(end_r, "tp", ahead)
        got_l = lax.ppermute(end_l, "tp", back)
        m = 2 * (n - 2)
        dx, *dw = pl.pallas_call(
            functools.partial(copy_kernel, n),
            out_shape=[shape(T, D)] + dws,
            in_specs=[hbm] + [vmem] * 5,
            out_specs=[hbm] * 4,
            scratch_shapes=[pltpu.VMEM((m, R, D // 2), BF), dma((m,)), dma((m,)), dma((5,))],
            compiler_params=pltpu.CompilerParams(vmem_limit_bytes=10 << 20),
            cost_estimate=pl.CostEstimate(flops=13_000_000_000, bytes_accessed=41_000_000, transcendentals=0),
            name="place",
        )(pltpu.with_memory_space_constraint(dx, pltpu.HBM), end_r, end_l, *dw)
        dx = pl.pallas_call(
            functools.partial(end_kernel, n),
            out_shape=shape(T, D),
            in_specs=[any_, vmem, vmem],
            out_specs=any_,
            scratch_shapes=[dma((2, 1))],
            input_output_aliases={0: 0},
            compiler_params=pltpu.CompilerParams(vmem_limit_bytes=1 << 20),
            name="place_end",
        )(dx, got_r, got_l)
        return dx, *dw

    tokens, columns, rows = P("dp", None), P(None, "tp"), P("tp", None)
    return jax.shard_map(
        step,
        mesh=mesh,
        in_specs=(tokens, tokens, P("dp", "tp"), P("dp", "tp"), columns, columns, rows),
        out_specs=(tokens, P("dp", "tp"), P("dp", "tp"), P(("dp", "tp"), None)),
        check_vma=False,
    )
```
